16 devices in a mesh: dp: 2 (over y, z), tp: 8 (over x, core).
Axes of the slice: x: 4, y: 2, z: 1, core: 2. Of those that a mesh axis runs over, the one named last changes fastest.
The devices are a block of a 4x4x8 slice.
Arguments:
- hidden: bfloat16 [32, 24, 4096], P('dp'), parts along dimension 0
- tree_mask: int32 [32, 24, 24], P('dp'), parts along dimension 0
- depth: int32 [32, 24], P('dp'), parts along dimension 0
- ctx_len: int32 [32], P('dp'), parts along dimension 0
- block_table: int32 [32, 12], P('dp'), parts along dimension 0
- score_id: int32 [32, 24], P('dp'), parts along dimension 0
- k_cache: bfloat16 [384, 16, 32, 128], P('dp', None, 'tp'), parts along dimension 0
- v_cache: bfloat16 [384, 16, 32, 128], P('dp', None, 'tp'), parts along dimension 0
- attn_norm: bfloat16 [4096], replicated
- w_q: bfloat16 [4096, 4096], P(None, 'tp')
- w_k: bfloat16 [4096, 4096], P(None, 'tp')
- w_v: bfloat16 [4096, 4096], P(None, 'tp')
- w_o: bfloat16 [4096, 4096], P('tp')
- mlp_norm: bfloat16 [4096], replicated
- w_gate: bfloat16 [4096, 11008], P(None, 'tp')
- w_up: bfloat16 [4096, 11008], P(None, 'tp')
- w_down: bfloat16 [11008, 4096], P('tp')
- final_norm: bfloat16 [4096], replicated
- w_lm: bfloat16 [4096, 32000], P(None, 'tp')
Outputs:
- output 1: float32 [32, 24], P('dp'), parts along dimension 0
- output 2: float32 [32, 24], P('dp'), parts along dimension 0
- output 3: bfloat16 [384, 16, 32, 128], P('dp', None, 'tp'), parts along dimension 0
- output 4: bfloat16 [384, 16, 32, 128], P('dp', None, 'tp'), parts along dimension 0
There are 2 independent parts. The reference program is written for one: setup_inputs(seed, part) draws one part's arguments, and reference() takes and returns one part's arrays. A program takes and returns all parts, laid end to end along the dimension named above; an argument that names none is the same for every part.
All inputs are finite; a program needn't handle non-finite values.
Results may differ from the reference program's by a relative error of at most 0.00375906.
Values are sent between devices in bfloat16 or wider.
A program may use at most 768 MiB of HBM per device.

```python
import math
import jax
import jax.numpy as jnp
from jax import lax

REQUESTS = 16
NODES = 24
PAGES = 12
PAGE_SIZE = 16
MODEL_DIM = 4096
HEADS = 32
KV_HEADS = 32
HEAD_DIM = 128
FFN_DIM = 11008
VOCAB_SIZE = 32000
ROPE_THETA = 500000
RMS_EPS = 1e-5
BLOCKS = REQUESTS * PAGES
SPAN = PAGES * PAGE_SIZE
MAX_CTX = SPAN - NODES
GROUP = HEADS // KV_HEADS


def draw_routing(key):
    k_spread, k_step, k_ctx, k_table, k_score = jax.random.split(key, 5)
    spread = jax.random.randint(k_spread, (REQUESTS, 1), 1, 4)
    step = jnp.minimum(jax.random.randint(k_step, (REQUESTS, NODES), 0, 4), spread)
    node_ids = jnp.arange(NODES)
    parent = jnp.maximum(node_ids[None, :] - 1 - step, 0)
    linked = (parent[:, :, None] == node_ids[None, None, :]) & (node_ids[None, :, None] > 0)
    reach = linked | (node_ids[:, None] == node_ids[None, :])[None]
    for _ in range(int(math.log2(NODES)) + 1):
        reach = jnp.any(reach[:, :, :, None] & reach[:, None, :, :], axis=2)
    tree_mask = reach.astype(jnp.int32)
    depth = jnp.sum(tree_mask, axis=-1).astype(jnp.int32) - 1
    ctx_len = jax.random.randint(k_ctx, (REQUESTS,), 1, MAX_CTX + 1).astype(jnp.int32)
    ctx_len = ctx_len.at[0].set(MAX_CTX)
    block_table = jax.random.permutation(k_table, BLOCKS).astype(jnp.int32).reshape(REQUESTS, PAGES)
    score_id = jax.random.randint(k_score, (REQUESTS, NODES), 0, VOCAB_SIZE).astype(jnp.int32)
    score_id = score_id.at[0, 0].set(VOCAB_SIZE - 1)
    return tree_mask, depth, ctx_len, block_table, score_id


def normal_weight(key, shape, scale):
    return (scale * jax.random.normal(key, shape, jnp.float32)).astype(jnp.bfloat16)


def gain_vector(key):
    return (1.0 + 0.3 * jax.random.normal(key, (MODEL_DIM,), jnp.float32)).astype(jnp.bfloat16)


def setup_inputs(seed: int = 0, part: int = 0) -> dict:
    part_key = jax.random.fold_in(jax.random.key(seed), part)
    keys = jax.random.split(part_key, 4)
    tree_mask, depth, ctx_len, block_table, score_id = draw_routing(keys[0])
    shared = jax.random.split(jax.random.key(seed + 1), 11)
    cache_shape = (BLOCKS, PAGE_SIZE, KV_HEADS, HEAD_DIM)
    return {
        "hidden": normal_weight(keys[1], (REQUESTS, NODES, MODEL_DIM), 1.0),
        "tree_mask": tree_mask,
        "depth": depth,
        "ctx_len": ctx_len,
        "block_table": block_table,
        "score_id": score_id,
        "k_cache": normal_weight(keys[2], cache_shape, 1.0),
        "v_cache": normal_weight(keys[3], cache_shape, 1.0),
        "attn_norm": gain_vector(shared[0]),
        "w_q": normal_weight(shared[1], (MODEL_DIM, HEADS * HEAD_DIM), 2.5 * MODEL_DIM ** -0.5),
        "w_k": normal_weight(shared[2], (MODEL_DIM, KV_HEADS * HEAD_DIM), 1.5 * MODEL_DIM ** -0.5),
        "w_v": normal_weight(shared[3], (MODEL_DIM, KV_HEADS * HEAD_DIM), MODEL_DIM ** -0.5),
        "w_o": normal_weight(shared[4], (HEADS * HEAD_DIM, MODEL_DIM), 1.5 * (HEADS * HEAD_DIM) ** -0.5),
        "mlp_norm": gain_vector(shared[5]),
        "w_gate": normal_weight(shared[6], (MODEL_DIM, FFN_DIM), MODEL_DIM ** -0.5),
        "w_up": normal_weight(shared[7], (MODEL_DIM, FFN_DIM), MODEL_DIM ** -0.5),
        "w_down": normal_weight(shared[8], (FFN_DIM, MODEL_DIM), 1.5 * FFN_DIM ** -0.5),
        "final_norm": gain_vector(shared[9]),
        "w_lm": normal_weight(shared[10], (MODEL_DIM, VOCAB_SIZE), 3.0 * MODEL_DIM ** -0.5),
    }


def rms_norm(values, gain):
    widened = values.astype(jnp.float32)
    scale = lax.rsqrt(jnp.mean(widened * widened, axis=-1, keepdims=True) + RMS_EPS)
    return (widened * scale * gain.astype(jnp.float32)).astype(jnp.bfloat16)


def rotate(values, positions):
    head_dim = values.shape[-1]
    half = head_dim // 2
    inv_freq = 1.0 / (ROPE_THETA ** (jnp.arange(half, dtype=jnp.float32) * (2.0 / head_dim)))
    angles = positions.astype(jnp.float32)[..., None] * inv_freq
    cosine = jnp.cos(angles)[..., None, :]
    sine = jnp.sin(angles)[..., None, :]
    first = values[..., :half]
    second = values[..., half:]
    return jnp.concatenate([first * cosine - second * sine, second * cosine + first * sine], axis=-1)


def reference(hidden, tree_mask, depth, ctx_len, block_table, score_id, k_cache, v_cache, attn_norm, w_q, w_k, w_v, w_o, mlp_norm, w_gate, w_up, w_down, final_norm, w_lm):
    scale = HEAD_DIM ** -0.5
    slot_ids = jnp.arange(SPAN)

    def one_request(item):
        rows, mask_row, depth_row, context, table_row, targets = item
        normed = rms_norm(rows, attn_norm)
        positions = context + depth_row
        query = jnp.dot(normed, w_q, preferred_element_type=jnp.float32).reshape(NODES, HEADS, HEAD_DIM)
        query = rotate(query, positions).astype(jnp.bfloat16).reshape(NODES, KV_HEADS, GROUP, HEAD_DIM)
        key_new = jnp.dot(normed, w_k, preferred_element_type=jnp.float32).reshape(NODES, KV_HEADS, HEAD_DIM)
        key_new = rotate(key_new, positions).astype(jnp.bfloat16)
        val_new = jnp.dot(normed, w_v, preferred_element_type=jnp.float32).astype(jnp.bfloat16).reshape(NODES, KV_HEADS, HEAD_DIM)
        key_old = k_cache[table_row].reshape(SPAN, KV_HEADS, HEAD_DIM)
        val_old = v_cache[table_row].reshape(SPAN, KV_HEADS, HEAD_DIM)
        query_wide = query.astype(jnp.float32)
        score_old = jnp.einsum("tkgh,skh->tkgs", query_wide, key_old.astype(jnp.float32)) * scale
        score_old = jnp.where((slot_ids < context)[None, None, None, :], score_old, -jnp.inf)
        score_new = jnp.einsum("tkgh,jkh->tkgj", query_wide, key_new.astype(jnp.float32)) * scale
        score_new = jnp.where((mask_row > 0)[:, None, None, :], score_new, -jnp.inf)
        top = jnp.maximum(jnp.max(score_old, axis=-1), jnp.max(score_new, axis=-1))[..., None]
        prob_old = jnp.exp(score_old - top)
        prob_new = jnp.exp(score_new - top)
        total = jnp.sum(prob_old, axis=-1) + jnp.sum(prob_new, axis=-1)
        mixed = jnp.einsum("tkgs,skh->tkgh", prob_old.astype(jnp.bfloat16).astype(jnp.float32), val_old.astype(jnp.float32))
        mixed = mixed + jnp.einsum("tkgj,jkh->tkgh", prob_new.astype(jnp.bfloat16).astype(jnp.float32), val_new.astype(jnp.float32))
        attended = (mixed / total[..., None]).astype(jnp.bfloat16).reshape(NODES, HEADS * HEAD_DIM)
        attn_out = jnp.dot(attended, w_o, preferred_element_type=jnp.float32).astype(jnp.bfloat16)
        residual = (rows.astype(jnp.float32) + attn_out.astype(jnp.float32)).astype(jnp.bfloat16)
        normed_mlp = rms_norm(residual, mlp_norm)
        gate = jnp.dot(normed_mlp, w_gate, preferred_element_type=jnp.float32)
        upper = jnp.dot(normed_mlp, w_up, preferred_element_type=jnp.float32)
        product = (jax.nn.silu(gate) * upper).astype(jnp.bfloat16)
        mlp_out = jnp.dot(product, w_down, preferred_element_type=jnp.float32).astype(jnp.bfloat16)
        layer_out = (residual.astype(jnp.float32) + mlp_out.astype(jnp.float32)).astype(jnp.bfloat16)
        logits = jnp.dot(rms_norm(layer_out, final_norm), w_lm, preferred_element_type=jnp.float32)
        log_norm = jax.nn.logsumexp(logits, axis=-1)
        picked = jnp.take_along_axis(logits, targets[:, None], axis=-1)[:, 0]
        return log_norm, picked - log_norm, key_new, val_new

    log_norm, log_prob, key_new, val_new = lax.map(one_request, (hidden, tree_mask, depth, ctx_len, block_table, score_id))
    slots = ctx_len[:, None] + jnp.arange(NODES)[None, :]
    slot_blocks = jnp.take_along_axis(block_table, slots // PAGE_SIZE, axis=1)
    k_out = k_cache.at[slot_blocks, slots % PAGE_SIZE].set(key_new)
    v_out = v_cache.at[slot_blocks, slots % PAGE_SIZE].set(val_new)
    return (log_norm, log_prob, k_out, v_out)
```

```python
import functools

import jax
import jax.numpy as jnp
import numpy as np
from jax import lax
from jax.experimental import pallas as pl
from jax.experimental.pallas import tpu as pltpu
from jax.sharding import PartitionSpec as P

RMS_EPS = 1e-5
ROPE_THETA = 500000
CHUNKS = (384,)
TILE = 256
VMEM_LIMIT = 66_000_000
HBM = pl.BlockSpec(memory_space=pl.ANY)
VMEM = pl.BlockSpec(memory_space=pltpu.VMEM)
LAST = (((1,), (1,)), ((), ()))
SMEM = pl.BlockSpec(memory_space=pltpu.SMEM)


def norm_rows(wide, gain):
    scale = lax.rsqrt(jnp.mean(wide * wide, axis=-1, keepdims=True) + RMS_EPS)
    return (wide * scale * gain).astype(jnp.bfloat16)


def attention_kernel(
    dims, ctx_ref, table_ref, hidden_hbm, gain_ref, cos_ref, sin_ref, mask_ref, wq_hbm, wk_hbm, wv_hbm, k_hbm, v_hbm,
    att_ref, k_out, v_out, hid, weights, kc, vc, q_buf, k_buf, v_buf, o_buf, in_sems, out_sems,
):
    requests, nodes, pages, page_rows, heads, head_dim = dims
    rows = requests * nodes
    stack = heads * nodes
    span_rows = pages * page_rows
    half_rows = rows // 2
    copies = []
    for part in range(2):
        piece = pl.ds(part * half_rows, half_rows)
        copies.append(pltpu.make_async_copy(hidden_hbm.at[piece], hid.at[piece], in_sems.at[part]))
    for i, w in enumerate((wq_hbm, wk_hbm, wv_hbm)):
        copies.append(pltpu.make_async_copy(w, weights.at[i], in_sems.at[2 + i]))
    copies.append(pltpu.make_async_copy(k_hbm, kc, in_sems.at[5]))
    copies.append(pltpu.make_async_copy(v_hbm, vc, in_sems.at[6]))
    for copy in copies:
        copy.start()

    gain = gain_ref[...].astype(jnp.float32)
    group = 16
    for part in range(2):
        copies[part].wait()

        def norm_step(i, _, part=part):
            piece = pl.ds(pl.multiple_of(part * half_rows + i * group, group), group)
            hid[piece, :] = norm_rows(hid[piece, :].astype(jnp.float32), gain)
            return 0

        lax.fori_loop(0, half_rows // group, norm_step, 0)

    width = heads * head_dim
    for i, buf in enumerate((q_buf, k_buf, v_buf)):
        copies[2 + i].wait()

        def project(t, _, i=i, buf=buf):
            cols = pl.ds(pl.multiple_of(t * TILE, TILE), TILE)
            out = jnp.dot(hid[...], weights[i, :, cols], preferred_element_type=jnp.float32)
            for h in range(TILE // head_dim):
                one = out[:, h * head_dim:(h + 1) * head_dim]
                if i < 2:
                    one = one * cos_ref[...] + pltpu.roll(one, head_dim // 2, 1) * sin_ref[...]
                one = one.astype(jnp.bfloat16).astype(jnp.float32)
                at = pl.ds(pl.multiple_of(t * TILE + h * head_dim, head_dim), head_dim)
                buf[:, at] = one
            return 0

        lax.fori_loop(0, width // TILE, project, 0)

    copies[5].wait()
    copies[6].wait()
    i32 = jnp.int32
    row_id = lax.broadcasted_iota(i32, (span_rows, 1), 0)
    stack_col = lax.broadcasted_iota(i32, (1, stack), 1)
    put = (stack_col % nodes) * heads + stack_col // nodes
    span_col = lax.broadcasted_iota(i32, (1, span_rows), 1)
    slot_col = span_col // heads
    stack_row = lax.broadcasted_iota(i32, (stack, 1), 0)
    same_head = (span_col % heads) == (stack_row // nodes)
    expand = ((stack_row % nodes) == lax.broadcasted_iota(i32, (1, nodes), 1)).astype(jnp.bfloat16)
    node_row = lax.broadcasted_iota(i32, (nodes, 1), 0)
    scale = head_dim ** -0.5

    def one_request(b):
        ctx = ctx_ref[b]
        at = [pl.ds(pl.multiple_of(table_ref[b, j] * page_rows, page_rows), page_rows) for j in range(pages)]
        mine = pl.ds(pl.multiple_of(b * nodes, 8), nodes)

        def stacked(buf):
            parts = [buf[mine, h * head_dim:(h + 1) * head_dim] for h in range(heads)]
            return jnp.concatenate(parts, axis=0).astype(jnp.bfloat16)

        place = (put + ctx * heads == row_id).astype(jnp.bfloat16)
        fresh = (row_id >= ctx * heads) & (row_id < ctx * heads + stack)

        def updated(cache, buf):
            old = jnp.concatenate([cache[p, :] for p in at], axis=0)
            new = jnp.dot(place, stacked(buf), preferred_element_type=jnp.float32)
            both = jnp.where(fresh, new, old.astype(jnp.float32)).astype(jnp.bfloat16)
            for j, p in enumerate(at):
                cache[p, :] = both[j * page_rows:(j + 1) * page_rows]
            return both

        keys = updated(kc, k_buf)
        vals = updated(vc, v_buf)
        score = lax.dot_general(stacked(q_buf), keys, (((1,), (1,)), ((), ())), preferred_element_type=jnp.float32) * scale
        tree = mask_ref[b].astype(jnp.float32).astype(jnp.bfloat16)
        tree = jnp.dot(expand, tree, preferred_element_type=jnp.float32).astype(jnp.bfloat16)
        spread = ((slot_col - ctx) == node_row).astype(jnp.bfloat16)
        tree = jnp.dot(tree, spread, preferred_element_type=jnp.float32)
        seen = same_head & ((slot_col < ctx) | (tree > 0.5))
        score = jnp.where(seen, score, -jnp.inf)
        prob = jnp.exp(score - jnp.max(score, axis=-1, keepdims=True))
        total = jnp.sum(prob, axis=-1, keepdims=True)
        mixed = jnp.dot(prob.astype(jnp.bfloat16), vals, preferred_element_type=jnp.float32) / total
        for h in range(heads):
            o_buf[mine, h * head_dim:(h + 1) * head_dim] = mixed[h * nodes:(h + 1) * nodes]

    def request_step(b, _):
        one_request(b)
        return 0

    lax.fori_loop(0, requests, request_step, 0)
    outs = [pltpu.make_async_copy(kc, k_out, out_sems.at[0]), pltpu.make_async_copy(vc, v_out, out_sems.at[1])]
    for copy in outs:
        copy.start()
    att_ref[...] = o_buf[...].astype(jnp.bfloat16)
    for copy in outs:
        copy.wait()


def attention(hidden, tree_mask, ctx_len, block_table, cosine, sine, k_pages, v_pages, attn_norm, w_q, w_k, w_v, dims):
    requests, nodes, pages, page_rows, heads, head_dim = dims
    rows = requests * nodes
    model = hidden.shape[1]
    width = heads * head_dim
    bf16, f32 = jnp.bfloat16, jnp.float32
    scratch = [
        pltpu.VMEM((rows, model), bf16),
        pltpu.VMEM((3, model, width), bf16),
        pltpu.VMEM(k_pages.shape, bf16),
        pltpu.VMEM(v_pages.shape, bf16),
    ] + [pltpu.VMEM((rows, width), f32)] * 4 + [pltpu.SemaphoreType.DMA((7,)), pltpu.SemaphoreType.DMA((2,))]
    return pl.pallas_call(
        functools.partial(attention_kernel, dims),
        name="attend",
        out_shape=(
            jax.ShapeDtypeStruct((rows, width), bf16),
            jax.ShapeDtypeStruct(k_pages.shape, bf16),
            jax.ShapeDtypeStruct(v_pages.shape, bf16),
        ),
        in_specs=[SMEM, SMEM, HBM, VMEM, VMEM, VMEM, VMEM, HBM, HBM, HBM, HBM, HBM],
        out_specs=(VMEM, HBM, HBM),
        scratch_shapes=scratch,
        compiler_params=pltpu.CompilerParams(vmem_limit_bytes=VMEM_LIMIT),
    )(ctx_len, block_table, hidden, attn_norm, cosine, sine, tree_mask, w_q, w_k, w_v, k_pages, v_pages)


def tail_kernel(
    chips, att_ref, hid_hbm, mlp_gain_ref, fin_gain_ref, want_ref, wo_hbm, wg_hbm, wu_hbm, wd_hbm, lm_hbm,
    out_ref, part, sib_in, rel_l, rel_r, in_l, in_r, xg, act, hid_own, run_max, run_sum, run_pick, stats,
    send_sems, recv_sems, stat_send, stat_recv, w_sems, lm_sems, hid_sems,
):
    f32, bf16 = jnp.float32, jnp.bfloat16
    rows, model = xg.shape
    ffn = wg_hbm.shape[0]
    vocab = lm_hbm.shape[0]
    half = model // 2
    members = 2 * chips
    me = lax.axis_index("tp")
    x = me // 2
    core = me % 2
    right = lax.rem(x + 1, chips) * 2 + core
    left = lax.rem(x + chips - 1, chips) * 2 + core
    sib = x * 2 + 1 - core
    offsets = [sum(CHUNKS[:i]) for i in range(len(CHUNKS))]

    barrier = pltpu.get_barrier_semaphore()
    for k in range(1, members):
        pl.semaphore_signal(barrier, inc=1, device_id={"tp": lax.rem(me + k, members)}, device_id_type=pl.DeviceIdType.MESH)

    def block(ch, hop, c=None):
        size = CHUNKS[ch] // members
        which = (core if c is None else c) * chips + lax.rem(x + hop + chips, chips)
        return pl.ds(pl.multiple_of(offsets[ch] + which * size, 16), size)

    def mine(ch):
        size = CHUNKS[ch] // members
        return pl.ds(offsets[ch] // members, size)

    def cols(h):
        return pl.ds(h * half, half)

    def remote(phase, ch, slot, src, dst, to):
        return pltpu.make_async_remote_copy(
            src_ref=src, dst_ref=dst, send_sem=send_sems.at[phase, ch, slot], recv_sem=recv_sems.at[phase, ch, slot],
            device_id={"tp": to}, device_id_type=pl.DeviceIdType.MESH,
        )

    def plan(phase, ch):
        size = CHUNKS[ch] // members
        quarter = size * chips
        far = pl.ds(pl.multiple_of(offsets[ch] + (1 - core) * quarter, 16), quarter)
        near = pl.ds(offsets[ch] // 2, quarter)
        own, opp, rgt, lft = block(ch, 0), block(ch, 2), block(ch, 1), block(ch, -1)
        m = mine(ch)
        h0, h1 = cols(0), cols(1)
        entries = [
            ("pair0", part.at[far, h0], sib_in.at[near, h0], sib),
            ("pair1", part.at[far, h1], sib_in.at[near, h1], sib),
            ("relay_r", part.at[opp, h0], rel_l.at[m, :], right),
            ("relay_l", part.at[opp, h1], rel_r.at[m, :], left),
            ("direct_r", part.at[rgt, h1], in_l.at[m, h1], right),
            ("direct_l", part.at[lft, h0], in_r.at[m, h0], left),
            ("acc_r", part.at[rgt, h0], in_l.at[m, h0], right),
            ("acc_l", part.at[lft, h1], in_r.at[m, h1], left),
            ("own_r0", xg.at[own, h0], xg.at[own, h0], right),
            ("own_r1", xg.at[own, h1], xg.at[own, h1], right),
            ("own_l0", xg.at[own, h0], xg.at[own, h0], left),
            ("own_l1", xg.at[own, h1], xg.at[own, h1], left),
            ("own_s", xg.at[own, :], xg.at[own, :], sib),
            ("fwd_r", xg.at[lft, h0], xg.at[lft, h0], right),
            ("fwd_l", xg.at[rgt, h1], xg.at[rgt, h1], left),
            ("lft_s", xg.at[lft, :], xg.at[lft, :], sib),
            ("rgt_s", xg.at[rgt, :], xg.at[rgt, :], sib),
            ("opp_s", xg.at[opp, :], xg.at[opp, :], sib),
        ]
        return {name: remote(phase, ch, i, src, dst, to) for i, (name, src, dst, to) in enumerate(entries)}

    reduce_names = ("pair0", "pair1", "relay_r", "relay_l", "direct_r", "direct_l", "acc_r", "acc_l")
    gather_names = ("own_r0", "own_r1", "own_l0", "own_l1", "own_s", "fwd_r", "fwd_l", "lft_s", "rgt_s", "opp_s")
    plans = [[plan(phase, ch) for ch in range(len(CHUNKS))] for phase in range(2)]

    def pair_sum(phase, ch):
        p = plans[phase][ch]
        quarter = CHUNKS[ch] // 2
        for h in range(2):
            p[f"pair{h}"].wait_recv()

            def add(i, _, h=h):
                there = pl.ds(pl.multiple_of(offsets[ch] + core * quarter + i * 16, 16), 16)
                here = pl.ds(pl.multiple_of(offsets[ch] // 2 + i * 16, 16), 16)
                total = part[there, cols(h)].astype(f32) + sib_in[here, cols(h)].astype(f32)
                part[there, cols(h)] = total.astype(bf16)
                return 0

            lax.fori_loop(0, quarter // 16, add, 0)
            if h == 0:
                p["relay_r"].start()
                p["direct_l"].start()
            else:
                p["relay_l"].start()
                p["direct_r"].start()

    def accumulate(phase, ch):
        p = plans[phase][ch]
        m = mine(ch)
        p["relay_r"].wait_recv()
        at = block(ch, 1)
        part[at, cols(0)] = (part[at, cols(0)].astype(f32) + rel_l[m, :].astype(f32)).astype(bf16)
        p["acc_r"].start()
        p["relay_l"].wait_recv()
        at = block(ch, -1)
        part[at, cols(1)] = (part[at, cols(1)].astype(f32) + rel_r[m, :].astype(f32)).astype(bf16)
        p["acc_l"].start()

    def finish(phase, ch, gain_ref):
        p = plans[phase][ch]
        for name in ("direct_r", "direct_l", "acc_r", "acc_l"):
            p[name].wait_recv()
        size = CHUNKS[ch] // members
        for i in range(size // 16):
            first = offsets[ch] + (core * chips + x) * size + i * 16
            there = pl.ds(pl.multiple_of(first, 16), 16)
            here = pl.ds(offsets[ch] // members + i * 16, 16)
            total = part[there, :].astype(f32) + in_l[here, :].astype(f32) + in_r[here, :].astype(f32)
            residual = (hid_own[here, :].astype(f32) + total.astype(bf16).astype(f32)).astype(bf16)
            if phase == 0:
                hid_own[here, :] = residual
            xg[there, :] = norm_rows(residual.astype(f32), gain_ref[...].astype(f32))
        for name in ("own_r0", "own_l1", "own_r1", "own_l0", "own_s"):
            p[name].start()

    def forward(phase, ch):
        p = plans[phase][ch]
        p["own_r0"].wait_recv()
        p["fwd_r"].start()
        p["own_l1"].wait_recv()
        p["fwd_l"].start()

    def share(phase, ch):
        p = plans[phase][ch]
        p["own_r1"].wait_recv()
        p["lft_s"].start()
        p["own_l0"].wait_recv()
        p["rgt_s"].start()
        p["fwd_r"].wait_recv()
        p["fwd_l"].wait_recv()
        p["opp_s"].start()

    def settle(phase, ch):
        p = plans[phase][ch]
        for name in ("own_s", "lft_s", "rgt_s", "opp_s"):
            p[name].wait_recv()
        for name in reduce_names + gather_names:
            p[name].wait_send()

    def chunk_rows(ch):
        return pl.ds(offsets[ch], CHUNKS[ch])

    def project(phase, ch, lhs_ref, w_ref):
        for h in range(2):
            def tile(t, _, h=h):
                at = pl.ds(pl.multiple_of(h * half + t * TILE, TILE), TILE)
                part[chunk_rows(ch), at] = jnp.dot(
                    lhs_ref[chunk_rows(ch), :], w_ref[:, at], preferred_element_type=f32
                ).astype(bf16)
                return 0

            lax.fori_loop(0, half // TILE, tile, 0)
            plans[phase][ch][f"pair{h}"].start()

    nch = len(CHUNKS)

    def layer(wo, wg, wu, wd):
        loads = [
            pltpu.make_async_copy(src, dst, w_sems.at[i])
            for i, (src, dst) in enumerate(((wo_hbm, wo), (wg_hbm, wg), (wu_hbm, wu), (wd_hbm, wd)))
        ]
        loads[0].start()
        own_rows = []
        for ch in range(nch):
            own_rows.append(pltpu.make_async_copy(hid_hbm.at[block(ch, 0), :], hid_own.at[mine(ch), :], hid_sems.at[ch]))
            own_rows[-1].start()
        loads[0].wait()
        for load in loads[1:]:
            load.start()
        pl.semaphore_wait(barrier, members - 1)
        for ch in range(nch):
            project(0, ch, att_ref, wo)
            if ch > 0:
                pair_sum(0, ch - 1)
        pair_sum(0, nch - 1)
        for copy in own_rows:
            copy.wait()
        for ch in range(nch):
            accumulate(0, ch)
        for ch in range(nch):
            finish(0, ch, mlp_gain_ref)
        for ch in range(nch):
            forward(0, ch)
        for load in loads[1:]:
            load.wait()

        def gated(ch):
            def tile(at):
                lhs = xg[chunk_rows(ch), :]
                gate = lax.dot_general(lhs, wg[at, :], LAST, preferred_element_type=f32)
                upper = lax.dot_general(lhs, wu[at, :], LAST, preferred_element_type=f32)
                act[chunk_rows(ch), at] = (gate * jax.nn.sigmoid(gate) * upper).astype(bf16)

            def step(t, _):
                tile(pl.ds(pl.multiple_of(t * TILE, TILE), TILE))
                return 0

            full = ffn // TILE
            lax.fori_loop(0, full, step, 0)
            if ffn % TILE:
                tile(pl.ds(full * TILE, ffn % TILE))

        for ch in range(nch):
            share(0, ch)
            settle(0, ch)
            gated(ch)
            if ch > 0:
                accumulate(1, ch - 1)
            project(1, ch, act, wd)
            if ch > 0:
                finish(1, ch - 1, fin_gain_ref)
            pair_sum(1, ch)

    ffn_shape = (ffn, model)
    pl.run_scoped(
        layer,
        pltpu.VMEM(wo_hbm.shape, bf16), pltpu.VMEM(ffn_shape, bf16), pltpu.VMEM(ffn_shape, bf16), pltpu.VMEM((ffn, model), bf16),
    )

    pieces = 5

    def head(lm):
        loads = []
        step_rows = vocab // pieces
        for i in range(pieces):
            piece = pl.ds(i * step_rows, step_rows)
            loads.append(pltpu.make_async_copy(lm_hbm.at[piece, :], lm.at[piece, :], lm_sems.at[i]))
            loads[-1].start()
        accumulate(1, nch - 1)
        if nch > 1:
            forward(1, 0)
        finish(1, nch - 1, fin_gain_ref)
        for ch in range(1 if nch > 1 else 0, nch):
            forward(1, ch)
        for load in loads:
            load.wait()
        group = 512
        full = vocab // group
        lanes = 128

        def logits(ch, at):
            return lax.dot_general(xg[chunk_rows(ch), :], lm[at, :], LAST, preferred_element_type=f32)

        def gather_tile(ch, values, base):
            r = chunk_rows(ch)
            parts = [values[:, i * lanes:(i + 1) * lanes] for i in range(values.shape[1] // lanes)]
            old = run_max[r, :]
            new = functools.reduce(jnp.maximum, parts, old)
            lane = lax.broadcasted_iota(jnp.int32, (1, lanes), 1) + base + me * vocab
            want = want_ref[r, :]
            total = run_sum[r, :] * jnp.exp(old - new)
            pick = run_pick[r, :]
            for i, one in enumerate(parts):
                total = total + jnp.exp(one - new)
                pick = pick + jnp.where(lane + i * lanes == want, one, 0.0)
            run_max[r, :] = new
            run_sum[r, :] = total
            run_pick[r, :] = pick

        for ch in range(nch):
            share(1, ch)
            settle(1, ch)
            r = chunk_rows(ch)
            run_max[r, :] = jnp.full((CHUNKS[ch], lanes), -jnp.inf, f32)
            run_sum[r, :] = jnp.zeros((CHUNKS[ch], lanes), f32)
            run_pick[r, :] = jnp.zeros((CHUNKS[ch], lanes), f32)

            def step(t, _, ch=ch):
                base = pl.multiple_of(t * group, group)
                gather_tile(ch, logits(ch, pl.ds(base, group)), base)
                return 0

            lax.fori_loop(0, full, step, 0)
            rest = vocab % group
            whole = rest // lanes * lanes
            last = logits(ch, pl.ds(full * group, rest))
            gather_tile(ch, last[:, :whole], full * group)
            end = last[:, whole:]
            top = jnp.maximum(jnp.max(run_max[r, :], axis=-1, keepdims=True), jnp.max(end, axis=-1, keepdims=True))
            total = jnp.sum(run_sum[r, :] * jnp.exp(run_max[r, :] - top), axis=-1, keepdims=True)
            total = total + jnp.sum(jnp.exp(end - top), axis=-1, keepdims=True)
            lane = lax.broadcasted_iota(jnp.int32, (1, rest - whole), 1) + (full * group + whole) + me * vocab
            pick = jnp.sum(run_pick[r, :], axis=-1, keepdims=True)
            pick = pick + jnp.sum(jnp.where(lane == want_ref[r, 0:1], end, 0.0), axis=-1, keepdims=True)
            place = lax.broadcasted_iota(jnp.int32, (1, lanes), 1)
            packed = jnp.where(place == 0, top, jnp.where(place == 1, total, pick))
            stats[me, :, r] = packed.T[0:8, :]

    pl.run_scoped(head, pltpu.VMEM((vocab, model), bf16))

    sends = []
    for k in range(1, members):
        to = lax.rem(me + k, members)
        sends.append(pltpu.make_async_remote_copy(
            src_ref=stats.at[me], dst_ref=stats.at[me], send_sem=stat_send.at[k - 1], recv_sem=stat_recv.at[k - 1],
            device_id={"tp": to}, device_id_type=pl.DeviceIdType.MESH,
        ))
        sends[-1].start()
    for copy in sends:
        copy.wait()
    every = [stats[i] for i in range(members)]
    top = functools.reduce(jnp.maximum, [e[0:1, :] for e in every])
    total = functools.reduce(jnp.add, [e[1:2, :] * jnp.exp(e[0:1, :] - top) for e in every])
    pick = functools.reduce(jnp.add, [e[2:3, :] for e in every])
    log_norm = top + jnp.log(total)
    out_ref[0:1, :] = log_norm
    out_ref[1:2, :] = pick - log_norm


def tail(attended, hidden, mlp_norm, final_norm, want, w_o, w_gate, w_up, w_down, w_lm, chips):
    rows, model = hidden.shape
    ffn = w_gate.shape[0]
    members = 2 * chips
    bf16, f32 = jnp.bfloat16, jnp.float32
    nch = len(CHUNKS)
    own = rows // members
    scratch = [
        pltpu.VMEM((rows, model), bf16),
        pltpu.VMEM((rows // 2, model), bf16),
        pltpu.VMEM((own, model // 2), bf16),
        pltpu.VMEM((own, model // 2), bf16),
        pltpu.VMEM((own, model), bf16),
        pltpu.VMEM((own, model), bf16),
        pltpu.VMEM((rows, model), bf16),
        pltpu.VMEM((rows, ffn), bf16),
        pltpu.VMEM((own, model), bf16),
        pltpu.VMEM((rows, 128), f32),
        pltpu.VMEM((rows, 128), f32),
        pltpu.VMEM((rows, 128), f32),
        pltpu.VMEM((members, 8, rows), f32),
        pltpu.SemaphoreType.DMA((2, nch, 18)),
        pltpu.SemaphoreType.DMA((2, nch, 18)),
        pltpu.SemaphoreType.DMA((members - 1,)),
        pltpu.SemaphoreType.DMA((members - 1,)),
        pltpu.SemaphoreType.DMA((4,)),
        pltpu.SemaphoreType.DMA((8,)),
        pltpu.SemaphoreType.DMA((nch,)),
    ]
    return pl.pallas_call(
        functools.partial(tail_kernel, chips),
        name="tail",
        out_shape=jax.ShapeDtypeStruct((2, rows), f32),
        in_specs=[VMEM, HBM, VMEM, VMEM, VMEM, HBM, HBM, HBM, HBM, HBM],
        out_specs=VMEM,
        scratch_shapes=scratch,
        compiler_params=pltpu.CompilerParams(vmem_limit_bytes=VMEM_LIMIT, collective_id=0, has_side_effects=True),
    )(attended, hidden, mlp_norm, final_norm, want, w_o, w_gate, w_up, w_down, w_lm)


def solution(mesh):
    chips = mesh.shape["tp"] // 2

    def group_step(hidden, tree_mask, depth, ctx_len, block_table, score_id, k_cache, v_cache, attn_norm, w_q, w_k, w_v, w_o, mlp_norm, w_gate, w_up, w_down, final_norm, w_lm):
        requests, nodes, model = hidden.shape
        blocks, page_size, heads, head_dim = k_cache.shape
        dims = (requests, nodes, block_table.shape[1], page_size * heads, heads, head_dim)
        rows = requests * nodes
        flat = hidden.reshape(rows, model)
        half = head_dim // 2
        inv_freq = 1.0 / (ROPE_THETA ** (jnp.arange(half, dtype=jnp.float32) * (2.0 / head_dim)))
        positions = (ctx_len[:, None] + depth).astype(jnp.float32).reshape(rows, 1)
        angles = positions * jnp.concatenate([inv_freq, inv_freq])[None, :]
        cosine = jnp.cos(angles)
        sine = jnp.sin(angles) * jnp.where(jnp.arange(head_dim) < half, -1.0, 1.0)[None, :]
        pages = (blocks * page_size * heads, head_dim)
        attended, k_out, v_out = attention(
            flat, tree_mask, ctx_len, block_table, cosine, sine, k_cache.reshape(pages), v_cache.reshape(pages),
            attn_norm.reshape(1, model), w_q, w_k, w_v, dims,
        )
        want = jnp.broadcast_to(score_id.reshape(rows, 1), (rows, 128))
        out = tail(attended, flat, mlp_norm.reshape(1, model), final_norm.reshape(1, model), want, w_o, w_gate.T, w_up.T, w_down, w_lm.T, chips)
        out = out.reshape(2, requests, nodes)
        return out[0], out[1], k_out.reshape(k_cache.shape), v_out.reshape(v_cache.shape)

    request_spec = P("dp", None, None)
    node_spec = P("dp", None)
    cache_spec = P("dp", None, "tp", None)
    shared_spec = P(None)
    column_spec = P(None, "tp")
    row_spec = P("tp", None)
    in_specs = (request_spec, request_spec, node_spec, P("dp"), node_spec, node_spec, cache_spec, cache_spec, shared_spec, column_spec, column_spec, column_spec, row_spec, shared_spec, column_spec, column_spec, row_spec, shared_spec, column_spec)
    out_specs = (node_spec, node_spec, cache_spec, cache_spec)
    return jax.shard_map(group_step, mesh=mesh, in_specs=in_specs, out_specs=out_specs, check_vma=False)
```

```python
import functools

import jax
import jax.numpy as jnp
import numpy as np
from jax import lax
from jax.experimental import pallas as pl
from jax.experimental.pallas import tpu as pltpu
from jax.sharding import PartitionSpec as P

RMS_EPS = 1e-5
ROPE_THETA = 500000
STEPS = 4
SPAN = 1024
GATE = 512
HEAD = 1024
TILE = 256
VMEM_LIMIT = 66_000_000
HBM = pl.BlockSpec(memory_space=pl.ANY)
VMEM = pl.BlockSpec(memory_space=pltpu.VMEM)
LAST = (((1,), (1,)), ((), ()))
SMEM = pl.BlockSpec(memory_space=pltpu.SMEM)


def norm_rows(wide, gain):
    scale = lax.rsqrt(jnp.mean(wide * wide, axis=-1, keepdims=True) + RMS_EPS)
    return (wide * scale * gain).astype(jnp.bfloat16)


def gain_row(ref):
    wide = ref[...].astype(jnp.float32)
    return jnp.concatenate([wide[i:i + 1, :] for i in range(wide.shape[0])], axis=1)


def column_of(ref, b):
    nodes = ref.shape[1]
    down = lax.broadcasted_iota(jnp.int32, (nodes, nodes), 0)
    across = lax.broadcasted_iota(jnp.int32, (nodes, nodes), 1)
    row = ref[pl.ds(b, 1), :].astype(jnp.float32)
    return jnp.sum(jnp.where(down == across, row, 0.0), axis=-1, keepdims=True)


def attention_kernel(
    dims, ctx_ref, table_ref, depth_ref, freq_ref, hidden_hbm, gain_ref, mask_ref, wq_hbm, wk_hbm, wv_hbm, k_hbm, v_hbm,
    att_ref, k_out, v_out, hid, normed, weights, kc, vc, cosine, sine, gain_buf, head_bias, q_buf, k_buf, v_buf, o_buf, in_sems, out_sems,
):
    requests, nodes, pages, page_rows, heads, head_dim = dims
    rows = requests * nodes
    stack = heads * nodes
    span_rows = pages * page_rows
    half_rows = rows // 2
    f32, bf16, i32 = jnp.float32, jnp.bfloat16, jnp.int32
    copies = []
    for part in range(2):
        piece = pl.ds(part * half_rows, half_rows)
        copies.append(pltpu.make_async_copy(hidden_hbm.at[piece], hid.at[piece], in_sems.at[part]))
    for i, w in enumerate((wq_hbm, wk_hbm, wv_hbm)):
        copies.append(pltpu.make_async_copy(w, weights.at[i], in_sems.at[2 + i]))
    copies.append(pltpu.make_async_copy(k_hbm, kc, in_sems.at[5]))
    copies.append(pltpu.make_async_copy(v_hbm, vc, in_sems.at[6]))
    for copy in copies:
        copy.start()

    gain_buf[...] = gain_row(gain_ref)
    lane = lax.broadcasted_iota(i32, (1, head_dim), 1)
    sign = jnp.where(lane < head_dim // 2, -1.0, 1.0)

    def angle_step(b, _):
        mine = pl.ds(pl.multiple_of(b * nodes, 8), nodes)
        angle = (column_of(depth_ref, b) + ctx_ref[b].astype(f32)) * freq_ref[...]
        cosine[mine, :] = jnp.cos(angle)
        sine[mine, :] = jnp.sin(angle) * sign
        return 0

    lax.fori_loop(0, requests, angle_step, 0)
    span_col = lax.broadcasted_iota(i32, (1, span_rows), 1)
    slot_col = span_col // heads
    stack_row = lax.broadcasted_iota(i32, (stack, 1), 0)
    stack_col = lax.broadcasted_iota(i32, (1, stack), 1)
    head_bias[...] = jnp.where((span_col % heads) == (stack_row // nodes), 0.0, -jnp.inf)

    group = 16
    for part in range(2):
        copies[part].wait()

        def norm_step(i, _, part=part):
            gain = gain_buf[...]
            at = [pl.ds(pl.multiple_of(part * half_rows + (i * 2 + k) * group, group), group) for k in range(2)]
            scales = []
            for p in at:
                wide = hid[p, :].astype(f32)
                scales.append(lax.rsqrt(jnp.mean(wide * wide, axis=-1, keepdims=True) + RMS_EPS))
            for p, scale in zip(at, scales):
                normed[p, :] = (hid[p, :].astype(f32) * scale * gain).astype(bf16)
            return 0

        lax.fori_loop(0, half_rows // group // 2, norm_step, 0)

    width = heads * head_dim
    for i, buf in enumerate((q_buf, k_buf, v_buf)):
        copies[2 + i].wait()

        def project(t, _, i=i, buf=buf):
            cols = pl.ds(pl.multiple_of(t * TILE, TILE), TILE)
            out = jnp.dot(normed[...], weights[i, :, cols], preferred_element_type=f32)
            for h in range(TILE // head_dim):
                one = out[:, h * head_dim:(h + 1) * head_dim]
                if i < 2:
                    one = one * cosine[...] + pltpu.roll(one, head_dim // 2, 1) * sine[...]
                one = one.astype(bf16).astype(f32)
                at = pl.ds(pl.multiple_of(t * TILE + h * head_dim, head_dim), head_dim)
                buf[:, at] = one
            return 0

        lax.fori_loop(0, width // TILE, project, 0)

    copies[5].wait()
    copies[6].wait()
    touched = -(-(nodes - 1) // (page_rows // heads)) + 1
    window = touched * page_rows
    row_id = lax.broadcasted_iota(i32, (window, 1), 0)
    put = (stack_col % nodes) * heads + stack_col // nodes
    expand = ((stack_row % nodes) == lax.broadcasted_iota(i32, (1, nodes), 1)).astype(bf16)
    spread = ((stack_col % nodes) == lax.broadcasted_iota(i32, (nodes, 1), 0)).astype(bf16)
    same_head = (stack_row // nodes) == (stack_col // nodes)
    scale = head_dim ** -0.5

    def attend(b):
        ctx = ctx_ref[b]
        at = [pl.ds(pl.multiple_of(table_ref[b, j] * page_rows, page_rows), page_rows) for j in range(pages)]
        mine = pl.ds(pl.multiple_of(b * nodes, 8), nodes)

        def stacked(buf):
            parts = [buf[mine, h * head_dim:(h + 1) * head_dim] for h in range(heads)]
            return jnp.concatenate(parts, axis=0).astype(bf16)

        query, key, val = stacked(q_buf), stacked(k_buf), stacked(v_buf)
        keys = jnp.concatenate([kc[p, :] for p in at], axis=0)
        vals = jnp.concatenate([vc[p, :] for p in at], axis=0)
        first = jnp.minimum(ctx // (page_rows // heads), pages - touched)
        shift = ctx * heads - first * page_rows
        place = (put + shift == row_id).astype(bf16)
        fresh = (row_id >= shift) & (row_id < shift + stack)
        new = jnp.dot(place, jnp.concatenate([key, val], axis=1), preferred_element_type=f32)
        tree = mask_ref[b].astype(f32).astype(bf16)
        tree = jnp.dot(expand, tree, preferred_element_type=f32).astype(bf16)
        tree = jnp.dot(tree, spread, preferred_element_type=f32)
        score = lax.dot_general(query, keys, LAST, preferred_element_type=f32) * scale
        slot_bias = jnp.where(slot_col < ctx, 0.0, -jnp.inf)
        score = score + (head_bias[...] + slot_bias)
        score_new = lax.dot_general(query, key, LAST, preferred_element_type=f32) * scale
        score_new = jnp.where(same_head & (tree > 0.5), score_new, -jnp.inf)
        top = jnp.maximum(jnp.max(score, axis=-1, keepdims=True), jnp.max(score_new, axis=-1, keepdims=True))
        prob = jnp.exp(score - top)
        prob_new = jnp.exp(score_new - top)
        total = jnp.sum(prob, axis=-1, keepdims=True) + jnp.sum(prob_new, axis=-1, keepdims=True)
        mixed = jnp.dot(prob.astype(bf16), vals, preferred_element_type=f32)
        mixed = (mixed + jnp.dot(prob_new.astype(bf16), val, preferred_element_type=f32)) / total
        stores = []
        for j in range(touched):
            page = pl.ds(pl.multiple_of(table_ref[b, first + j] * page_rows, page_rows), page_rows)
            piece = slice(j * page_rows, (j + 1) * page_rows)
            for c, cache in enumerate((kc, vc)):
                fill = new[piece, c * head_dim:(c + 1) * head_dim]
                old = cache[page, :].astype(f32)
                stores.append((cache, page, jnp.where(fresh[piece], fill, old).astype(bf16)))
        return mine, mixed, stores

    together = 4

    def request_step(i, _):
        done = [attend(i * together + k) for k in range(together)]
        for mine, mixed, stores in done:
            for h in range(heads):
                o_buf[mine, h * head_dim:(h + 1) * head_dim] = mixed[h * nodes:(h + 1) * nodes]
            for cache, page, value in stores:
                cache[page, :] = value
        return 0

    lax.fori_loop(0, requests // together, request_step, 0)
    outs = [pltpu.make_async_copy(kc, k_out, out_sems.at[0]), pltpu.make_async_copy(vc, v_out, out_sems.at[1])]
    for copy in outs:
        copy.start()
    att_ref[...] = o_buf[...].astype(bf16)
    for copy in outs:
        copy.wait()


def attention(hidden, tree_mask, depth, ctx_len, block_table, freq, k_pages, v_pages, attn_norm, w_q, w_k, w_v, dims):
    requests, nodes, pages, page_rows, heads, head_dim = dims
    rows = requests * nodes
    model = hidden.shape[1]
    width = heads * head_dim
    bf16, f32 = jnp.bfloat16, jnp.float32
    scratch = [
        pltpu.VMEM((rows, model), bf16),
        pltpu.VMEM((rows, model), bf16),
        pltpu.VMEM((3, model, width), bf16),
        pltpu.VMEM(k_pages.shape, bf16),
        pltpu.VMEM(v_pages.shape, bf16),
        pltpu.VMEM((rows, head_dim), f32),
        pltpu.VMEM((rows, head_dim), f32),
        pltpu.VMEM((1, model), f32),
        pltpu.VMEM((heads * nodes, pages * page_rows), f32),
    ] + [pltpu.VMEM((rows, width), f32)] * 4 + [pltpu.SemaphoreType.DMA((7,)), pltpu.SemaphoreType.DMA((2,))]
    return pl.pallas_call(
        functools.partial(attention_kernel, dims),
        name="attend",
        out_shape=(
            jax.ShapeDtypeStruct((rows, width), bf16),
            jax.ShapeDtypeStruct(k_pages.shape, bf16),
            jax.ShapeDtypeStruct(v_pages.shape, bf16),
        ),
        in_specs=[SMEM, SMEM, VMEM, VMEM, HBM, VMEM, VMEM, HBM, HBM, HBM, HBM, HBM],
        out_specs=(VMEM, HBM, HBM),
        scratch_shapes=scratch,
        compiler_params=pltpu.CompilerParams(vmem_limit_bytes=VMEM_LIMIT),
    )(ctx_len, block_table, depth, freq, hidden, attn_norm, tree_mask, w_q, w_k, w_v, k_pages, v_pages)


def tail_kernel(
    chips, att_ref, hid_hbm, mlp_gain_ref, fin_gain_ref, score_ref, wo_hbm, wg_hbm, wu_hbm, wd_hbm, lm_hbm,
    top_ref, total_ref, pick_ref, part, sib_in, rel_l, rel_r, in_l, in_r, xg, act, hid_own, run_max, run_sum, run_pick, stats, want_ref, gains,
    send_sems, recv_sems, stat_send, stat_recv, w_sems, lm_sems, hid_sem,
):
    f32, bf16 = jnp.float32, jnp.bfloat16
    rows, model = xg.shape
    ffn = wg_hbm.shape[0]
    vocab = lm_hbm.shape[0]
    members = 2 * chips
    size = rows // members
    quarter = size * chips
    wide = model // STEPS
    sub = wide // 2
    me = lax.axis_index("tp")
    x = me // 2
    core = me % 2
    right = lax.rem(x + 1, chips) * 2 + core
    left = lax.rem(x + chips - 1, chips) * 2 + core
    sib = x * 2 + 1 - core

    barrier = pltpu.get_barrier_semaphore()
    for k in range(1, members):
        pl.semaphore_signal(barrier, inc=1, device_id={"tp": lax.rem(me + k, members)}, device_id_type=pl.DeviceIdType.MESH)

    def first_row(hop):
        return (core * chips + lax.rem(x + hop + chips, chips)) * size

    def block(hop):
        return pl.ds(pl.multiple_of(first_row(hop), 16), size)

    def lanes_of(start, width):
        return pl.ds(start if isinstance(start, int) else pl.multiple_of(start, 128), width)

    def cols(c, part=None):
        if part is None:
            return lanes_of(c * wide, wide)
        return lanes_of(c * wide + part * sub, sub)

    def plan(phase, c, name):
        far = pl.ds(pl.multiple_of((1 - core) * quarter, 16), quarter)
        own, opp, rgt, lft = block(0), block(2), block(1), block(-1)
        both = cols(c)
        c0, c1, here = cols(c, 0), cols(c, 1), lanes_of(c * sub, sub)
        entries = [
            ("pair", part.at[far, both], sib_in.at[:, both], sib),
            ("relay_r", part.at[opp, c0], rel_l.at[:, here], right),
            ("relay_l", part.at[opp, c1], rel_r.at[:, here], left),
            ("direct_r", part.at[rgt, c1], in_l.at[:, c1], right),
            ("direct_l", part.at[lft, c0], in_r.at[:, c0], left),
            ("acc_r", part.at[rgt, c0], in_l.at[:, c0], right),
            ("acc_l", part.at[lft, c1], in_r.at[:, c1], left),
            ("own_r0", xg.at[own, c0], xg.at[own, c0], right),
            ("own_l1", xg.at[own, c1], xg.at[own, c1], left),
            ("own_r1", xg.at[own, c1], xg.at[own, c1], right),
            ("own_l0", xg.at[own, c0], xg.at[own, c0], left),
            ("own_s", xg.at[own, both], xg.at[own, both], sib),
            ("fwd_r", xg.at[lft, c0], xg.at[lft, c0], right),
            ("fwd_l", xg.at[rgt, c1], xg.at[rgt, c1], left),
            ("lft_s", xg.at[lft, both], xg.at[lft, both], sib),
            ("rgt_s", xg.at[rgt, both], xg.at[rgt, both], sib),
            ("opp_s", xg.at[opp, both], xg.at[opp, both], sib),
        ]
        i = [entry[0] for entry in entries].index(name)
        _, src, dst, to = entries[i]
        return pltpu.make_async_remote_copy(
            src_ref=src, dst_ref=dst, send_sem=send_sems.at[phase, c, i], recv_sem=recv_sems.at[phase, c, i],
            device_id={"tp": to}, device_id_type=pl.DeviceIdType.MESH,
        )

    reduce_names = ("pair", "relay_r", "relay_l", "direct_r", "direct_l", "acc_r", "acc_l")
    own_names = ("own_r0", "own_l1", "own_r1", "own_l0", "own_s")
    other_names = ("fwd_r", "fwd_l", "lft_s", "rgt_s", "opp_s")
    steps = range(STEPS)

    def pair_sum(phase, c):
        both = cols(c)
        plan(phase, c, "pair").wait_recv()

        def add(i, _):
            there = pl.ds(pl.multiple_of(core * quarter + i * 32, 16), 32)
            here = pl.ds(pl.multiple_of(i * 32, 32), 32)
            part[there, both] = (part[there, both].astype(f32) + sib_in[here, both].astype(f32)).astype(bf16)
            return 0

        lax.fori_loop(0, quarter // 32, add, 0)
        for name in ("relay_r", "relay_l", "direct_r", "direct_l"):
            plan(phase, c, name).start()

    def accumulate(phase, c):
        here = lanes_of(c * sub, sub)
        for name, hop, which, buf in (("r", 1, 0, rel_l), ("l", -1, 1, rel_r)):
            plan(phase, c, f"relay_{name}").wait_recv()
            at = block(hop)
            part[at, cols(c, which)] = (part[at, cols(c, which)].astype(f32) + buf[:, here].astype(f32)).astype(bf16)
            plan(phase, c, f"acc_{name}").start()

    def own_send(phase, c):
        for name in own_names:
            plan(phase, c, name).start()

    def finish(phase):
        squares = 0.0
        for c in steps:
            both = cols(c)
            for name in ("direct_r", "direct_l", "acc_r", "acc_l"):
                plan(phase, c, name).wait_recv()
            total = part[block(0), both].astype(f32) + in_l[:, both].astype(f32) + in_r[:, both].astype(f32)
            residual = (hid_own[:, both].astype(f32) + total.astype(bf16).astype(f32)).astype(bf16)
            hid_own[:, both] = residual
            full = residual.astype(f32)
            squares = squares + jnp.sum(full * full, axis=-1, keepdims=True)
        scale = lax.rsqrt(squares * (1.0 / model) + RMS_EPS)
        for c in steps:
            both = cols(c)
            xg[block(0), both] = (hid_own[:, both].astype(f32) * scale * gains[phase:phase + 1, both]).astype(bf16)
            if c < 2:
                own_send(phase, c)

    def forward(phase, c, more=True):
        plan(phase, c, "own_r0").wait_recv()
        plan(phase, c, "fwd_r").start()
        plan(phase, c, "own_l1").wait_recv()
        plan(phase, c, "fwd_l").start()
        if more:
            own_send(phase, c + 2)

    def share(phase, c):
        plan(phase, c, "own_r1").wait_recv()
        plan(phase, c, "lft_s").start()
        plan(phase, c, "own_l0").wait_recv()
        plan(phase, c, "rgt_s").start()
        plan(phase, c, "fwd_r").wait_recv()
        plan(phase, c, "fwd_l").wait_recv()
        plan(phase, c, "opp_s").start()

    def ready(phase, c):
        for name in ("own_s", "lft_s", "rgt_s", "opp_s"):
            plan(phase, c, name).wait_recv()

    def drain(phase):
        def one(c, _):
            for name in reduce_names + own_names + other_names:
                plan(phase, c, name).wait_send()
            return 0

        lax.fori_loop(0, STEPS, one, 0)

    def reduce(phase, lhs_ref, w_ref):
        def step(c, _):
            @pl.when(c < STEPS)
            def _():
                part[:, cols(c)] = jnp.dot(lhs_ref[...], w_ref[:, cols(c)], preferred_element_type=f32).astype(bf16)
                plan(phase, c, "pair").start()

            @pl.when((c >= 1) & (c <= STEPS))
            def _():
                pair_sum(phase, c - 1)

            @pl.when(c >= 3)
            def _():
                accumulate(phase, c - 3)

            return 0

        lax.fori_loop(0, STEPS + 3, step, 0)
        finish(phase)

    def gather(phase, compute, loads):
        forward(phase, 0)
        forward(phase, 1)
        share(phase, 0)
        ready(phase, 0)
        forward(phase, 2, False)
        for load in loads:
            load.wait()

        def step(c, _):
            compute(cols(c), False, 0)
            share(phase, c + 1)

            @pl.when(c == 0)
            def _():
                forward(phase, 3, False)

            compute(cols(c), False, 1)

            @pl.when(c == 1)
            def _():
                share(phase, 3)

            @pl.when(c == 0)
            def _():
                ready(phase, 1)

            return 0

        lax.fori_loop(0, 2, step, 0)
        ready(phase, 2)
        ready(phase, 3)
        compute(pl.ds(2 * wide, 2 * wide), True, None)

    def layer(wo, wg, wu, wd, gate_acc, up_acc):
        loads = [
            pltpu.make_async_copy(src, dst, w_sems.at[i])
            for i, (src, dst) in enumerate(((wo_hbm, wo), (wg_hbm, wg), (wu_hbm, wu), (wd_hbm, wd)))
        ]
        loads[0].start()
        own_rows = pltpu.make_async_copy(hid_hbm.at[block(0), :], hid_own, hid_sem.at[0])
        own_rows.start()
        gains[0:1, :] = gain_row(mlp_gain_ref)
        gains[1:2, :] = gain_row(fin_gain_ref)

        def want_step(b, _):
            nodes = score_ref.shape[1]
            column = column_of(score_ref, b).astype(jnp.int32)
            want_ref[pl.ds(pl.multiple_of(b * nodes, 8), nodes), :] = jnp.broadcast_to(column, (nodes, 128))
            return 0

        lax.fori_loop(0, score_ref.shape[0], want_step, 0)
        own_rows.wait()
        loads[0].wait()
        for load in loads[1:]:
            load.start()
        gate_acc[...] = jnp.zeros(gate_acc.shape, f32)
        up_acc[...] = jnp.zeros(up_acc.shape, f32)
        pl.semaphore_wait(barrier, members - 1)
        reduce(0, att_ref, wo)

        def gated(span, is_last, half):
            def close(start, width):
                at = pl.ds(start, width)
                gate = gate_acc[:, at]
                act[:, at] = (gate * jax.nn.sigmoid(gate) * up_acc[:, at]).astype(bf16)

            def tile(start, width):
                at = pl.ds(start, width)
                for w, acc in ((wg, gate_acc), (wu, up_acc)):
                    acc[:, at] += lax.dot_general(xg[:, span], w[at, span], LAST, preferred_element_type=f32)

            def step(t, _):
                tile(pl.multiple_of(t * GATE, GATE), GATE)
                return 0

            def last_step(t, _):
                tile(pl.multiple_of(t * GATE, GATE), GATE)
                close(pl.multiple_of((t - 1) * GATE, GATE), GATE)
                return 0

            full = ffn // GATE
            if is_last:
                tile(0, GATE)
                lax.fori_loop(1, full, last_step, 0)
                tile(full * GATE, ffn - full * GATE)
                close((full - 1) * GATE, GATE)
                close(full * GATE, ffn - full * GATE)
            elif half == 0:
                lax.fori_loop(0, full, step, 0)
            else:
                tile(full * GATE, ffn - full * GATE)

        gather(0, gated, loads[1:3])
        drain(0)
        loads[3].wait()
        reduce(1, act, wd)

    pl.run_scoped(
        layer,
        pltpu.VMEM(wo_hbm.shape, bf16), pltpu.VMEM((ffn, model), bf16), pltpu.VMEM((ffn, model), bf16), pltpu.VMEM((ffn, model), bf16),
        pltpu.VMEM((rows, ffn), f32), pltpu.VMEM((rows, ffn), f32),
    )

    pieces = 5
    lanes = 128

    def head(lm, acc):
        loads = []
        step_rows = vocab // pieces
        for i in range(pieces):
            piece = pl.ds(i * step_rows, step_rows)
            loads.append(pltpu.make_async_copy(lm_hbm.at[piece, :], lm.at[piece, :], lm_sems.at[i]))
            loads[-1].start()
        run_max[...] = jnp.full(run_max.shape, -jnp.inf, f32)
        run_sum[...] = jnp.zeros(run_sum.shape, f32)
        run_pick[...] = jnp.zeros(run_pick.shape, f32)
        full = vocab // HEAD
        rest = vocab % HEAD
        whole = rest // lanes * lanes

        def fold(base, width):
            parts = [acc[:, pl.ds(base + i * lanes, lanes)] for i in range(width // lanes)]
            old = run_max[...]
            new = functools.reduce(jnp.maximum, parts, old)
            lane = lax.broadcasted_iota(jnp.int32, (1, lanes), 1) + base + me * vocab
            want = want_ref[...]
            total = run_sum[...] * jnp.exp(old - new)
            pick = run_pick[...]
            for i, one in enumerate(parts):
                total = total + jnp.exp(one - new)
                pick = pick + jnp.where(lane + i * lanes == want, one, 0.0)
            run_max[...] = new
            run_sum[...] = total
            run_pick[...] = pick

        def logits(span, is_last, half):
            def tile(base, width):
                at = pl.ds(base, width)
                acc[:, at] += lax.dot_general(xg[:, span], lm[at, span], LAST, preferred_element_type=f32)

            def step(t, _):
                tile(pl.multiple_of(t * HEAD, HEAD), HEAD)
                if is_last:
                    fold(pl.multiple_of((t - 1) * HEAD, HEAD), HEAD)
                return 0

            cut = (full + 1) // 2
            if is_last:
                tile(0, HEAD)
                lax.fori_loop(1, full, step, 0)
                tile(full * HEAD, rest)
                fold((full - 1) * HEAD, HEAD)
            elif half == 0:
                lax.fori_loop(0, cut, step, 0)
            else:
                lax.fori_loop(cut, full, step, 0)
                tile(full * HEAD, rest)

        acc[...] = jnp.zeros(acc.shape, f32)
        gather(1, logits, loads)
        fold(full * HEAD, whole)
        end = acc[:, full * HEAD + whole:vocab]
        top = jnp.maximum(jnp.max(run_max[...], axis=-1, keepdims=True), jnp.max(end, axis=-1, keepdims=True))
        total = jnp.sum(run_sum[...] * jnp.exp(run_max[...] - top), axis=-1, keepdims=True)
        total = total + jnp.sum(jnp.exp(end - top), axis=-1, keepdims=True)
        lane = lax.broadcasted_iota(jnp.int32, (1, rest - whole), 1) + (full * HEAD + whole) + me * vocab
        pick = jnp.sum(run_pick[...], axis=-1, keepdims=True)
        pick = pick + jnp.sum(jnp.where(lane == want_ref[:, 0:1], end, 0.0), axis=-1, keepdims=True)
        place = lax.broadcasted_iota(jnp.int32, (1, lanes), 1)
        packed = jnp.where(place == 0, top, jnp.where(place == 1, total, pick))
        stats[me] = packed.T[0:8, :]

    pl.run_scoped(head, pltpu.VMEM((vocab, model), bf16), pltpu.VMEM((rows, vocab), f32))

    sends = []
    for k in range(1, members):
        to = lax.rem(me + k, members)
        sends.append(pltpu.make_async_remote_copy(
            src_ref=stats.at[me], dst_ref=stats.at[me], send_sem=stat_send.at[k - 1], recv_sem=stat_recv.at[k - 1],
            device_id={"tp": to}, device_id_type=pl.DeviceIdType.MESH,
        ))
        sends[-1].start()
    drain(1)
    for copy in sends:
        copy.wait()
    every = [stats[i] for i in range(members)]
    top = functools.reduce(jnp.maximum, [e[0:1, :] for e in every])
    total = functools.reduce(jnp.add, [e[1:2, :] * jnp.exp(e[0:1, :] - top) for e in every])
    pick = functools.reduce(jnp.add, [e[2:3, :] for e in every])
    requests, nodes = score_ref.shape
    for b in range(requests):
        for ref, row in ((top_ref, top), (total_ref, total), (pick_ref, pick)):
            ref[b:b + 1, :] = row[:, b * nodes:(b + 1) * nodes]


def tail(attended, hidden, mlp_norm, final_norm, score_id, w_o, w_gate, w_up, w_down, w_lm, chips):
    rows, model = hidden.shape
    ffn = w_gate.shape[0]
    members = 2 * chips
    bf16, f32 = jnp.bfloat16, jnp.float32
    own = rows // members
    scratch = [
        pltpu.VMEM((rows, model), bf16),
        pltpu.VMEM((rows // 2, model), bf16),
        pltpu.VMEM((own, model // 2), bf16),
        pltpu.VMEM((own, model // 2), bf16),
        pltpu.VMEM((own, model), bf16),
        pltpu.VMEM((own, model), bf16),
        pltpu.VMEM((rows, model), bf16),
        pltpu.VMEM((rows, ffn), bf16),
        pltpu.VMEM((own, model), bf16),
        pltpu.VMEM((rows, 128), f32),
        pltpu.VMEM((rows, 128), f32),
        pltpu.VMEM((rows, 128), f32),
        pltpu.VMEM((members, 8, rows), f32),
        pltpu.VMEM((rows, 128), jnp.int32),
        pltpu.VMEM((2, model), f32),
        pltpu.SemaphoreType.DMA((2, STEPS, 17)),
        pltpu.SemaphoreType.DMA((2, STEPS, 17)),
        pltpu.SemaphoreType.DMA((members - 1,)),
        pltpu.SemaphoreType.DMA((members - 1,)),
        pltpu.SemaphoreType.DMA((4,)),
        pltpu.SemaphoreType.DMA((5,)),
        pltpu.SemaphoreType.DMA((1,)),
    ]
    return pl.pallas_call(
        functools.partial(tail_kernel, chips),
        name="tail",
        out_shape=(jax.ShapeDtypeStruct(score_id.shape, f32),) * 3,
        in_specs=[VMEM, HBM, VMEM, VMEM, VMEM, HBM, HBM, HBM, HBM, HBM],
        out_specs=(VMEM, VMEM, VMEM),
        scratch_shapes=scratch,
        compiler_params=pltpu.CompilerParams(vmem_limit_bytes=VMEM_LIMIT, collective_id=0, has_side_effects=True),
    )(attended, hidden, mlp_norm, final_norm, score_id, w_o, w_gate, w_up, w_down, w_lm)


def solution(mesh):
    chips = mesh.shape["tp"] // 2

    def group_step(hidden, tree_mask, depth, ctx_len, block_table, score_id, k_cache, v_cache, attn_norm, w_q, w_k, w_v, w_o, mlp_norm, w_gate, w_up, w_down, final_norm, w_lm):
        requests, nodes, model = hidden.shape
        blocks, page_size, heads, head_dim = k_cache.shape
        dims = (requests, nodes, block_table.shape[1], page_size * heads, heads, head_dim)
        rows = requests * nodes
        flat = hidden.reshape(rows, model)
        half = head_dim // 2
        inv_freq = 1.0 / (ROPE_THETA ** (jnp.arange(half, dtype=jnp.float32) * (2.0 / head_dim)))
        freq = jnp.concatenate([inv_freq, inv_freq])[None, :]
        pages = (blocks * page_size * heads, head_dim)
        attended, k_out, v_out = attention(
            flat, tree_mask, depth, ctx_len, block_table, freq, k_cache.reshape(pages), v_cache.reshape(pages),
            attn_norm.reshape(model // 128, 128), w_q, w_k, w_v, dims,
        )
        top, total, pick = tail(
            attended, flat, mlp_norm.reshape(model // 128, 128), final_norm.reshape(model // 128, 128), score_id,
            w_o, w_gate.T, w_up.T, w_down, w_lm.T, chips,
        )
        log_norm = top + jnp.log(total)
        return log_norm, pick - log_norm, k_out.reshape(k_cache.shape), v_out.reshape(v_cache.shape)

    request_spec = P("dp", None, None)
    node_spec = P("dp", None)
    cache_spec = P("dp", None, "tp", None)
    shared_spec = P(None)
    column_spec = P(None, "tp")
    row_spec = P("tp", None)
    in_specs = (request_spec, request_spec, node_spec, P("dp"), node_spec, node_spec, cache_spec, cache_spec, shared_spec, column_spec, column_spec, column_spec, row_spec, shared_spec, column_spec, column_spec, row_spec, shared_spec, column_spec)
    out_specs = (node_spec, node_spec, cache_spec, cache_spec)
    return jax.shard_map(group_step, mesh=mesh, in_specs=in_specs, out_specs=out_specs, check_vma=False)
```

```python
import functools

import jax
import jax.numpy as jnp
import numpy as np
from jax import lax
from jax.experimental import pallas as pl
from jax.experimental.pallas import tpu as pltpu
from jax.sharding import PartitionSpec as P

RMS_EPS = 1e-5
ROPE_THETA = 500000
STEPS = 4
SPAN = 1024
GATE = 512
HEAD = 1024
TILE = 256
VMEM_LIMIT = 66_000_000
HBM = pl.BlockSpec(memory_space=pl.ANY)
VMEM = pl.BlockSpec(memory_space=pltpu.VMEM)
LAST = (((1,), (1,)), ((), ()))
SMEM = pl.BlockSpec(memory_space=pltpu.SMEM)


def norm_rows(wide, gain):
    scale = lax.rsqrt(jnp.mean(wide * wide, axis=-1, keepdims=True) + RMS_EPS)
    return (wide * scale * gain).astype(jnp.bfloat16)


def gain_row(ref):
    wide = ref[...].astype(jnp.float32)
    return jnp.concatenate([wide[i:i + 1, :] for i in range(wide.shape[0])], axis=1)


def window_pages(nodes, page_size):
    return -(-(nodes - 1) // page_size) + 1


def column_of(ref, b):
    nodes = ref.shape[1]
    down = lax.broadcasted_iota(jnp.int32, (nodes, nodes), 0)
    across = lax.broadcasted_iota(jnp.int32, (nodes, nodes), 1)
    row = ref[pl.ds(b, 1), :].astype(jnp.float32)
    return jnp.sum(jnp.where(down == across, row, 0.0), axis=-1, keepdims=True)


def attention_kernel(
    dims, ctx_ref, table_ref, depth_ref, freq_ref, hidden_hbm, gain_ref, mask_ref, wq_hbm, wk_hbm, wv_hbm, k_hbm, v_hbm,
    att_ref, k_out, v_out, hid, normed, weights, kc, vc, cosine, sine, gain_buf, head_bias, q_buf, k_buf, v_buf, o_buf, renewed, in_sems, out_sems,
):
    requests, nodes, pages, page_rows, heads, head_dim = dims
    rows = requests * nodes
    stack = heads * nodes
    span_rows = pages * page_rows
    half_rows = rows // 2
    f32, bf16, i32 = jnp.float32, jnp.bfloat16, jnp.int32
    copies = []
    for part in range(2):
        piece = pl.ds(part * half_rows, half_rows)
        copies.append(pltpu.make_async_copy(hidden_hbm.at[piece], hid.at[piece], in_sems.at[part]))
    for i, w in enumerate((wq_hbm, wk_hbm, wv_hbm)):
        copies.append(pltpu.make_async_copy(w, weights.at[i], in_sems.at[2 + i]))
    copies.append(pltpu.make_async_copy(k_hbm, kc, in_sems.at[5]))
    copies.append(pltpu.make_async_copy(v_hbm, vc, in_sems.at[6]))
    for copy in copies[:3]:
        copy.start()

    gain_buf[...] = gain_row(gain_ref)
    lane = lax.broadcasted_iota(i32, (1, head_dim), 1)
    sign = jnp.where(lane < head_dim // 2, -1.0, 1.0)

    def angle_step(b, _):
        mine = pl.ds(pl.multiple_of(b * nodes, 8), nodes)
        angle = (column_of(depth_ref, b) + ctx_ref[b].astype(f32)) * freq_ref[...]
        cosine[mine, :] = jnp.cos(angle)
        sine[mine, :] = jnp.sin(angle) * sign
        return 0

    lax.fori_loop(0, requests, angle_step, 0)
    for copy in copies[3:]:
        copy.start()
    span_col = lax.broadcasted_iota(i32, (1, span_rows), 1)
    slot_col = span_col // heads
    stack_row = lax.broadcasted_iota(i32, (stack, 1), 0)
    stack_col = lax.broadcasted_iota(i32, (1, stack), 1)
    head_bias[...] = jnp.where((span_col % heads) == (stack_row // nodes), 0.0, -jnp.inf)

    group = 16
    for part in range(2):
        copies[part].wait()

        def norm_step(i, _, part=part):
            gain = gain_buf[...]
            at = [pl.ds(pl.multiple_of(part * half_rows + (i * 2 + k) * group, group), group) for k in range(2)]
            scales = []
            for p in at:
                wide = hid[p, :].astype(f32)
                scales.append(lax.rsqrt(jnp.mean(wide * wide, axis=-1, keepdims=True) + RMS_EPS))
            for p, scale in zip(at, scales):
                normed[p, :] = (hid[p, :].astype(f32) * scale * gain).astype(bf16)
            return 0

        lax.fori_loop(0, half_rows // group // 2, norm_step, 0)

    flush = [pltpu.make_async_copy(cache, out, out_sems.at[k]) for k, (cache, out) in enumerate(((kc, k_out), (vc, v_out)))]
    width = heads * head_dim
    for i, buf in enumerate((q_buf, k_buf, v_buf)):
        copies[2 + i].wait()

        def project(t, _, i=i, buf=buf):
            cols = pl.ds(pl.multiple_of(t * TILE, TILE), TILE)
            out = jnp.dot(normed[...], weights[i, :, cols], preferred_element_type=f32)
            for h in range(TILE // head_dim):
                one = out[:, h * head_dim:(h + 1) * head_dim]
                if i < 2:
                    one = one * cosine[...] + pltpu.roll(one, head_dim // 2, 1) * sine[...]
                one = one.astype(bf16).astype(f32)
                at = pl.ds(pl.multiple_of(t * TILE + h * head_dim, head_dim), head_dim)
                buf[:, at] = one
            return 0

        lax.fori_loop(0, width // TILE, project, 0)
        if i == 1:
            for k, whole in enumerate(flush):
                copies[5 + k].wait()
                whole.start()

    touched = window_pages(nodes, page_rows // heads)
    window = touched * page_rows
    row_id = lax.broadcasted_iota(i32, (window, 1), 0)
    put = (stack_col % nodes) * heads + stack_col // nodes
    expand = ((stack_row % nodes) == lax.broadcasted_iota(i32, (1, nodes), 1)).astype(bf16)
    spread = ((stack_col % nodes) == lax.broadcasted_iota(i32, (nodes, 1), 0)).astype(bf16)
    same_head = (stack_row // nodes) == (stack_col // nodes)
    scale = head_dim ** -0.5

    def attend(b):
        ctx = ctx_ref[b]
        at = [pl.ds(pl.multiple_of(table_ref[b, j] * page_rows, page_rows), page_rows) for j in range(pages)]
        mine = pl.ds(pl.multiple_of(b * nodes, 8), nodes)

        def stacked(buf):
            parts = [buf[mine, h * head_dim:(h + 1) * head_dim] for h in range(heads)]
            return jnp.concatenate(parts, axis=0).astype(bf16)

        query, key, val = stacked(q_buf), stacked(k_buf), stacked(v_buf)
        keys = jnp.concatenate([kc[p, :] for p in at], axis=0)
        vals = jnp.concatenate([vc[p, :] for p in at], axis=0)
        first = jnp.minimum(ctx // (page_rows // heads), pages - touched)
        shift = ctx * heads - first * page_rows
        place = (put + shift == row_id).astype(bf16)
        fresh = (row_id >= shift) & (row_id < shift + stack)
        new = jnp.dot(place, jnp.concatenate([key, val], axis=1), preferred_element_type=f32)
        tree = mask_ref[b].astype(f32).astype(bf16)
        tree = jnp.dot(expand, tree, preferred_element_type=f32).astype(bf16)
        tree = jnp.dot(tree, spread, preferred_element_type=f32)
        score = lax.dot_general(query, keys, LAST, preferred_element_type=f32) * scale
        slot_bias = jnp.where(slot_col < ctx, 0.0, -jnp.inf)
        score = score + (head_bias[...] + slot_bias)
        score_new = lax.dot_general(query, key, LAST, preferred_element_type=f32) * scale
        score_new = jnp.where(same_head & (tree > 0.5), score_new, -jnp.inf)
        top = jnp.maximum(jnp.max(score, axis=-1, keepdims=True), jnp.max(score_new, axis=-1, keepdims=True))
        prob = jnp.exp(score - top)
        prob_new = jnp.exp(score_new - top)
        total = jnp.sum(prob, axis=-1, keepdims=True) + jnp.sum(prob_new, axis=-1, keepdims=True)
        mixed = jnp.dot(prob.astype(bf16), vals, preferred_element_type=f32)
        mixed = (mixed + jnp.dot(prob_new.astype(bf16), val, preferred_element_type=f32)) / total
        stores = []
        for j in range(touched):
            page = pl.ds(pl.multiple_of(table_ref[b, first + j] * page_rows, page_rows), page_rows)
            piece = slice(j * page_rows, (j + 1) * page_rows)
            for c, cache in enumerate((kc, vc)):
                fill = new[piece, c * head_dim:(c + 1) * head_dim]
                old = cache[page, :].astype(f32)
                stores.append((c, j, page, jnp.where(fresh[piece], fill, old).astype(bf16)))
        return mine, mixed, stores

    together = 4
    for whole in flush:
        whole.wait()

    def request_step(i, _):
        done = [attend(i * together + k) for k in range(together)]
        for k, (mine, mixed, stores) in enumerate(done):
            for h in range(heads):
                o_buf[mine, h * head_dim:(h + 1) * head_dim] = mixed[h * nodes:(h + 1) * nodes]
            for c, j, page, value in stores:
                slot = pl.ds(pl.multiple_of((i * together + k) * window + j * page_rows, page_rows), page_rows)
                renewed[c, slot, :] = value
        for k, (mine, mixed, stores) in enumerate(done):
            for c, j, page, value in stores:
                slot = pl.ds(pl.multiple_of((i * together + k) * window + j * page_rows, page_rows), page_rows)
                out = (k_out, v_out)[c]
                pltpu.make_async_copy(renewed.at[c, slot, :], out.at[page, :], out_sems.at[2 + c]).start()
        return 0

    lax.fori_loop(0, requests // together, request_step, 0)
    att_ref[...] = o_buf[...].astype(bf16)
    for c, out in enumerate((k_out, v_out)):
        pltpu.make_async_copy(renewed.at[c], out.at[pl.ds(0, requests * window), :], out_sems.at[2 + c]).wait()


def attention(hidden, tree_mask, depth, ctx_len, block_table, freq, k_pages, v_pages, attn_norm, w_q, w_k, w_v, dims):
    requests, nodes, pages, page_rows, heads, head_dim = dims
    rows = requests * nodes
    model = hidden.shape[1]
    width = heads * head_dim
    bf16, f32 = jnp.bfloat16, jnp.float32
    window = window_pages(nodes, page_rows // heads) * page_rows
    scratch = [
        pltpu.VMEM((rows, model), bf16),
        pltpu.VMEM((rows, model), bf16),
        pltpu.VMEM((3, model, width), bf16),
        pltpu.VMEM(k_pages.shape, bf16),
        pltpu.VMEM(v_pages.shape, bf16),
        pltpu.VMEM((rows, head_dim), f32),
        pltpu.VMEM((rows, head_dim), f32),
        pltpu.VMEM((1, model), f32),
        pltpu.VMEM((heads * nodes, pages * page_rows), f32),
    ] + [pltpu.VMEM((rows, width), f32)] * 4 + [pltpu.VMEM((2, requests * window, head_dim), bf16), pltpu.SemaphoreType.DMA((7,)), pltpu.SemaphoreType.DMA((4,))]
    return pl.pallas_call(
        functools.partial(attention_kernel, dims),
        name="attend",
        out_shape=(
            jax.ShapeDtypeStruct((rows, width), bf16),
            jax.ShapeDtypeStruct(k_pages.shape, bf16),
            jax.ShapeDtypeStruct(v_pages.shape, bf16),
        ),
        in_specs=[SMEM, SMEM, VMEM, VMEM, HBM, VMEM, VMEM, HBM, HBM, HBM, HBM, HBM],
        out_specs=(VMEM, HBM, HBM),
        scratch_shapes=scratch,
        compiler_params=pltpu.CompilerParams(vmem_limit_bytes=VMEM_LIMIT),
    )(ctx_len, block_table, depth, freq, hidden, attn_norm, tree_mask, w_q, w_k, w_v, k_pages, v_pages)


def tail_kernel(
    chips, att_ref, hid_hbm, mlp_gain_ref, fin_gain_ref, score_ref, wo_hbm, wg_hbm, wu_hbm, wd_hbm, lm_hbm,
    top_ref, total_ref, pick_ref, part, sib_in, rel_l, rel_r, in_l, in_r, xg, act, hid_own, run_max, run_sum, run_pick, stats, want_ref, gains,
    send_sems, recv_sems, stat_send, stat_recv, w_sems, wo_sems, lm_sems, hid_sem,
):
    f32, bf16 = jnp.float32, jnp.bfloat16
    rows, model = xg.shape
    ffn = wg_hbm.shape[0]
    vocab = lm_hbm.shape[0]
    members = 2 * chips
    size = rows // members
    quarter = size * chips
    wide = model // STEPS
    sub = wide // 2
    me = lax.axis_index("tp")
    x = me // 2
    core = me % 2
    right = lax.rem(x + 1, chips) * 2 + core
    left = lax.rem(x + chips - 1, chips) * 2 + core
    sib = x * 2 + 1 - core

    barrier = pltpu.get_barrier_semaphore()
    for k in range(1, members):
        pl.semaphore_signal(barrier, inc=1, device_id={"tp": lax.rem(me + k, members)}, device_id_type=pl.DeviceIdType.MESH)

    def first_row(hop):
        return (core * chips + lax.rem(x + hop + chips, chips)) * size

    def block(hop):
        return pl.ds(pl.multiple_of(first_row(hop), 16), size)

    def lanes_of(start, width):
        return pl.ds(start if isinstance(start, int) else pl.multiple_of(start, 128), width)

    def cols(c, part=None):
        if part is None:
            return lanes_of(c * wide, wide)
        return lanes_of(c * wide + part * sub, sub)

    def plan(phase, c, name):
        far = pl.ds(pl.multiple_of((1 - core) * quarter, 16), quarter)
        own, opp, rgt, lft = block(0), block(2), block(1), block(-1)
        both = cols(c)
        c0, c1, here = cols(c, 0), cols(c, 1), lanes_of(c * sub, sub)
        entries = [
            ("pair", part.at[far, both], sib_in.at[:, both], sib),
            ("relay_r", part.at[opp, c0], rel_l.at[:, here], right),
            ("relay_l", part.at[opp, c1], rel_r.at[:, here], left),
            ("direct_r", part.at[rgt, c1], in_l.at[:, c1], right),
            ("direct_l", part.at[lft, c0], in_r.at[:, c0], left),
            ("acc_r", part.at[rgt, c0], in_l.at[:, c0], right),
            ("acc_l", part.at[lft, c1], in_r.at[:, c1], left),
            ("own_r0", xg.at[own, c0], xg.at[own, c0], right),
            ("own_l1", xg.at[own, c1], xg.at[own, c1], left),
            ("own_r1", xg.at[own, c1], xg.at[own, c1], right),
            ("own_l0", xg.at[own, c0], xg.at[own, c0], left),
            ("own_s", xg.at[own, both], xg.at[own, both], sib),
            ("fwd_r", xg.at[lft, c0], xg.at[lft, c0], right),
            ("fwd_l", xg.at[rgt, c1], xg.at[rgt, c1], left),
            ("lft_s", xg.at[lft, both], xg.at[lft, both], sib),
            ("rgt_s", xg.at[rgt, both], xg.at[rgt, both], sib),
            ("opp_s", xg.at[opp, both], xg.at[opp, both], sib),
        ]
        i = [entry[0] for entry in entries].index(name)
        _, src, dst, to = entries[i]
        return pltpu.make_async_remote_copy(
            src_ref=src, dst_ref=dst, send_sem=send_sems.at[phase, c, i], recv_sem=recv_sems.at[phase, c, i],
            device_id={"tp": to}, device_id_type=pl.DeviceIdType.MESH,
        )

    reduce_names = ("pair", "relay_r", "relay_l", "direct_r", "direct_l", "acc_r", "acc_l")
    own_names = ("own_r0", "own_l1", "own_r1", "own_l0", "own_s")
    other_names = ("fwd_r", "fwd_l", "lft_s", "rgt_s", "opp_s")
    steps = range(STEPS)

    def pair_sum(phase, c):
        both = cols(c)
        plan(phase, c, "pair").wait_recv()

        def add(i, _):
            there = pl.ds(pl.multiple_of(core * quarter + i * 32, 16), 32)
            here = pl.ds(pl.multiple_of(i * 32, 32), 32)
            part[there, both] = (part[there, both].astype(f32) + sib_in[here, both].astype(f32)).astype(bf16)
            return 0

        lax.fori_loop(0, quarter // 32, add, 0)
        for name in ("relay_r", "relay_l", "direct_r", "direct_l"):
            plan(phase, c, name).start()

    def accumulate(phase, c):
        here = lanes_of(c * sub, sub)
        for name, hop, which, buf in (("r", 1, 0, rel_l), ("l", -1, 1, rel_r)):
            plan(phase, c, f"relay_{name}").wait_recv()
            at = block(hop)
            part[at, cols(c, which)] = (part[at, cols(c, which)].astype(f32) + buf[:, here].astype(f32)).astype(bf16)
            plan(phase, c, f"acc_{name}").start()

    def own_send(phase, c):
        for name in own_names:
            plan(phase, c, name).start()

    def finish(phase):
        squares = 0.0
        for c in steps:
            both = cols(c)
            for name in ("direct_r", "direct_l", "acc_r", "acc_l"):
                plan(phase, c, name).wait_recv()
            total = part[block(0), both].astype(f32) + in_l[:, both].astype(f32) + in_r[:, both].astype(f32)
            residual = (hid_own[:, both].astype(f32) + total.astype(bf16).astype(f32)).astype(bf16)
            hid_own[:, both] = residual
            full = residual.astype(f32)
            squares = squares + jnp.sum(full * full, axis=-1, keepdims=True)
        scale = lax.rsqrt(squares * (1.0 / model) + RMS_EPS)
        for c in steps:
            both = cols(c)
            xg[block(0), both] = (hid_own[:, both].astype(f32) * scale * gains[phase:phase + 1, both]).astype(bf16)
            if c < 2:
                own_send(phase, c)

    def forward(phase, c, more=True):
        plan(phase, c, "own_r0").wait_recv()
        plan(phase, c, "fwd_r").start()
        plan(phase, c, "own_l1").wait_recv()
        plan(phase, c, "fwd_l").start()
        if more:
            own_send(phase, c + 2)

    def share(phase, c):
        plan(phase, c, "own_r1").wait_recv()
        plan(phase, c, "lft_s").start()
        plan(phase, c, "own_l0").wait_recv()
        plan(phase, c, "rgt_s").start()
        plan(phase, c, "fwd_r").wait_recv()
        plan(phase, c, "fwd_l").wait_recv()
        plan(phase, c, "opp_s").start()

    def ready(phase, c):
        for name in ("own_s", "lft_s", "rgt_s", "opp_s"):
            plan(phase, c, name).wait_recv()

    def drain(phase):
        def one(c, _):
            for name in reduce_names + own_names + other_names:
                plan(phase, c, name).wait_send()
            return 0

        lax.fori_loop(0, STEPS, one, 0)

    def reduce(phase, lhs_ref, w_ref, before, filler):
        def step(c, _):
            @pl.when(c < STEPS)
            def _():
                before(c)
                part[:, cols(c)] = jnp.dot(lhs_ref[...], w_ref[:, cols(c)], preferred_element_type=f32).astype(bf16)
                plan(phase, c, "pair").start()

            @pl.when((c >= 1) & (c <= STEPS))
            def _():
                pair_sum(phase, c - 1)

            @pl.when(c >= 3)
            def _():
                accumulate(phase, c - 3)

            return 0

        lax.fori_loop(0, STEPS + 3, step, 0)
        filler()
        finish(phase)

    def gather(phase, compute, loads):
        forward(phase, 0)
        forward(phase, 1)
        share(phase, 0)
        ready(phase, 0)
        forward(phase, 2, False)
        for load in loads:
            load.wait()

        def step(c, _):
            compute(cols(c), False, 0)
            share(phase, c + 1)

            @pl.when(c == 0)
            def _():
                forward(phase, 3, False)

            compute(cols(c), False, 1)

            @pl.when(c == 1)
            def _():
                share(phase, 3)

            @pl.when(c == 0)
            def _():
                ready(phase, 1)

            return 0

        lax.fori_loop(0, 2, step, 0)
        ready(phase, 2)
        ready(phase, 3)
        compute(pl.ds(2 * wide, 2 * wide), True, None)

    def layer(wo, wg, wu, wd, gate_acc, up_acc):
        loads = [
            pltpu.make_async_copy(src, dst, w_sems.at[i])
            for i, (src, dst) in enumerate(((wg_hbm, wg), (wu_hbm, wu), (wd_hbm, wd)))
        ]
        def wo_piece(c):
            return pltpu.make_async_copy(wo_hbm.at[:, cols(c)], wo.at[:, cols(c)], wo_sems.at[c])

        for c in steps:
            wo_piece(c).start()
        own_rows = pltpu.make_async_copy(hid_hbm.at[block(0), :], hid_own, hid_sem.at[0])
        own_rows.start()

        def before(c):
            wo_piece(c).wait()

            @pl.when(c == STEPS - 1)
            def _():
                for load in loads:
                    load.start()

        def filler():
            gains[0:1, :] = gain_row(mlp_gain_ref)
            gains[1:2, :] = gain_row(fin_gain_ref)
            gate_acc[...] = jnp.zeros(gate_acc.shape, f32)
            up_acc[...] = jnp.zeros(up_acc.shape, f32)
            own_rows.wait()

        pl.semaphore_wait(barrier, members - 1)
        reduce(0, att_ref, wo, before, filler)

        def gated(span, is_last, half):
            def close(start, width):
                at = pl.ds(start, width)
                gate = gate_acc[:, at]
                act[:, at] = (gate * jax.nn.sigmoid(gate) * up_acc[:, at]).astype(bf16)

            def tile(start, width):
                at = pl.ds(start, width)
                for w, acc in ((wg, gate_acc), (wu, up_acc)):
                    acc[:, at] += lax.dot_general(xg[:, span], w[at, span], LAST, preferred_element_type=f32)

            def step(t, _):
                tile(pl.multiple_of(t * GATE, GATE), GATE)
                return 0

            full = ffn // GATE
            if is_last:
                pieces = [(t * GATE, min(GATE, ffn - t * GATE)) for t in range(-(-ffn // GATE))]
                tile(*pieces[0])
                for t in range(1, len(pieces)):
                    close(*pieces[t - 1])
                    tile(*pieces[t])
                close(*pieces[-1])
            elif half == 0:
                lax.fori_loop(0, full, step, 0)
            else:
                tile(full * GATE, ffn - full * GATE)

        gather(0, gated, loads[:2])
        drain(0)
        loads[2].wait()
        reduce(1, act, wd, lambda c: None, lambda: None)

    pl.run_scoped(
        layer,
        pltpu.VMEM(wo_hbm.shape, bf16), pltpu.VMEM((ffn, model), bf16), pltpu.VMEM((ffn, model), bf16), pltpu.VMEM((ffn, model), bf16),
        pltpu.VMEM((rows, ffn), f32), pltpu.VMEM((rows, ffn), f32),
    )

    pieces = 5
    lanes = 128

    def head(lm, acc):
        loads = []
        step_rows = vocab // pieces
        for i in range(pieces):
            piece = pl.ds(i * step_rows, step_rows)
            loads.append(pltpu.make_async_copy(lm_hbm.at[piece, :], lm.at[piece, :], lm_sems.at[i]))
            loads[-1].start()

        def want_step(b, _):
            nodes = score_ref.shape[1]
            column = column_of(score_ref, b).astype(jnp.int32)
            want_ref[pl.ds(pl.multiple_of(b * nodes, 8), nodes), :] = jnp.broadcast_to(column, (nodes, 128))
            return 0

        lax.fori_loop(0, score_ref.shape[0], want_step, 0)
        run_max[...] = jnp.full(run_max.shape, -jnp.inf, f32)
        run_sum[...] = jnp.zeros(run_sum.shape, f32)
        run_pick[...] = jnp.zeros(run_pick.shape, f32)
        full = vocab // HEAD
        rest = vocab % HEAD
        whole = rest // lanes * lanes

        def fold(base, width):
            parts = [acc[:, pl.ds(base + i * lanes, lanes)] for i in range(width // lanes)]
            old = run_max[...]
            new = functools.reduce(jnp.maximum, parts, old)
            lane = lax.broadcasted_iota(jnp.int32, (1, lanes), 1) + base + me * vocab
            want = want_ref[...]
            total = run_sum[...] * jnp.exp(old - new)
            pick = run_pick[...]
            for i, one in enumerate(parts):
                total = total + jnp.exp(one - new)
                pick = pick + jnp.where(lane + i * lanes == want, one, 0.0)
            run_max[...] = new
            run_sum[...] = total
            run_pick[...] = pick

        def logits(span, is_last, half):
            def tile(base, width):
                at = pl.ds(base, width)
                acc[:, at] += lax.dot_general(xg[:, span], lm[at, span], LAST, preferred_element_type=f32)

            def step(t, _):
                tile(pl.multiple_of(t * HEAD, HEAD), HEAD)
                return 0

            cut = (full + 1) // 2
            if is_last:
                for t in range(full):
                    tile(t * HEAD, HEAD)
                    if t > 0:
                        fold((t - 1) * HEAD, HEAD)
                fold((full - 1) * HEAD, HEAD)
                tile(full * HEAD, rest)
            elif half == 0:
                lax.fori_loop(0, cut, step, 0)
            else:
                lax.fori_loop(cut, full, step, 0)
                tile(full * HEAD, rest)

        acc[...] = jnp.zeros(acc.shape, f32)
        gather(1, logits, loads)
        fold(full * HEAD, whole)
        end = acc[:, full * HEAD + whole:vocab]
        top = jnp.maximum(jnp.max(run_max[...], axis=-1, keepdims=True), jnp.max(end, axis=-1, keepdims=True))
        total = jnp.sum(run_sum[...] * jnp.exp(run_max[...] - top), axis=-1, keepdims=True)
        total = total + jnp.sum(jnp.exp(end - top), axis=-1, keepdims=True)
        lane = lax.broadcasted_iota(jnp.int32, (1, rest - whole), 1) + (full * HEAD + whole) + me * vocab
        pick = jnp.sum(run_pick[...], axis=-1, keepdims=True)
        pick = pick + jnp.sum(jnp.where(lane == want_ref[:, 0:1], end, 0.0), axis=-1, keepdims=True)
        place = lax.broadcasted_iota(jnp.int32, (1, lanes), 1)
        packed = jnp.where(place == 0, top, jnp.where(place == 1, total, pick))
        stats[me] = packed.T[0:8, :]

    pl.run_scoped(head, pltpu.VMEM((vocab, model), bf16), pltpu.VMEM((rows, vocab), f32))

    sends = []
    for k in range(1, members):
        to = lax.rem(me + k, members)
        sends.append(pltpu.make_async_remote_copy(
            src_ref=stats.at[me], dst_ref=stats.at[me], send_sem=stat_send.at[k - 1], recv_sem=stat_recv.at[k - 1],
            device_id={"tp": to}, device_id_type=pl.DeviceIdType.MESH,
        ))
        sends[-1].start()
    drain(1)
    for copy in sends:
        copy.wait()
    every = [stats[i] for i in range(members)]
    top = functools.reduce(jnp.maximum, [e[0:1, :] for e in every])
    total = functools.reduce(jnp.add, [e[1:2, :] * jnp.exp(e[0:1, :] - top) for e in every])
    pick = functools.reduce(jnp.add, [e[2:3, :] for e in every])
    requests, nodes = score_ref.shape
    for b in range(requests):
        for ref, row in ((top_ref, top), (total_ref, total), (pick_ref, pick)):
            ref[b:b + 1, :] = row[:, b * nodes:(b + 1) * nodes]


def tail(attended, hidden, mlp_norm, final_norm, score_id, w_o, w_gate, w_up, w_down, w_lm, chips):
    rows, model = hidden.shape
    ffn = w_gate.shape[0]
    members = 2 * chips
    bf16, f32 = jnp.bfloat16, jnp.float32
    own = rows // members
    scratch = [
        pltpu.VMEM((rows, model), bf16),
        pltpu.VMEM((rows // 2, model), bf16),
        pltpu.VMEM((own, model // 2), bf16),
        pltpu.VMEM((own, model // 2), bf16),
        pltpu.VMEM((own, model), bf16),
        pltpu.VMEM((own, model), bf16),
        pltpu.VMEM((rows, model), bf16),
        pltpu.VMEM((rows, ffn), bf16),
        pltpu.VMEM((own, model), bf16),
        pltpu.VMEM((rows, 128), f32),
        pltpu.VMEM((rows, 128), f32),
        pltpu.VMEM((rows, 128), f32),
        pltpu.VMEM((members, 8, rows), f32),
        pltpu.VMEM((rows, 128), jnp.int32),
        pltpu.VMEM((2, model), f32),
        pltpu.SemaphoreType.DMA((2, STEPS, 17)),
        pltpu.SemaphoreType.DMA((2, STEPS, 17)),
        pltpu.SemaphoreType.DMA((members - 1,)),
        pltpu.SemaphoreType.DMA((members - 1,)),
        pltpu.SemaphoreType.DMA((3,)),
        pltpu.SemaphoreType.DMA((STEPS,)),
        pltpu.SemaphoreType.DMA((5,)),
        pltpu.SemaphoreType.DMA((1,)),
    ]
    return pl.pallas_call(
        functools.partial(tail_kernel, chips),
        name="tail",
        out_shape=(jax.ShapeDtypeStruct(score_id.shape, f32),) * 3,
        in_specs=[VMEM, HBM, VMEM, VMEM, VMEM, HBM, HBM, HBM, HBM, HBM],
        out_specs=(VMEM, VMEM, VMEM),
        scratch_shapes=scratch,
        compiler_params=pltpu.CompilerParams(vmem_limit_bytes=VMEM_LIMIT, collective_id=0, has_side_effects=True),
    )(attended, hidden, mlp_norm, final_norm, score_id, w_o, w_gate, w_up, w_down, w_lm)


def solution(mesh):
    chips = mesh.shape["tp"] // 2

    def group_step(hidden, tree_mask, depth, ctx_len, block_table, score_id, k_cache, v_cache, attn_norm, w_q, w_k, w_v, w_o, mlp_norm, w_gate, w_up, w_down, final_norm, w_lm):
        requests, nodes, model = hidden.shape
        blocks, page_size, heads, head_dim = k_cache.shape
        dims = (requests, nodes, block_table.shape[1], page_size * heads, heads, head_dim)
        rows = requests * nodes
        flat = hidden.reshape(rows, model)
        inv_freq = 1.0 / (ROPE_THETA ** (np.arange(head_dim // 2) * (2.0 / head_dim)))
        freq = jnp.asarray(np.concatenate([inv_freq, inv_freq])[None, :], jnp.float32)
        pages = (blocks * page_size * heads, head_dim)
        attended, k_out, v_out = attention(
            flat, tree_mask, depth, ctx_len, block_table, freq, k_cache.reshape(pages), v_cache.reshape(pages),
            attn_norm.reshape(model // 128, 128), w_q, w_k, w_v, dims,
        )
        top, total, pick = tail(
            attended, flat, mlp_norm.reshape(model // 128, 128), final_norm.reshape(model // 128, 128), score_id,
            w_o, w_gate.T, w_up.T, w_down, w_lm.T, chips,
        )
        log_norm = top + jnp.log(total)
        return log_norm, pick - log_norm, k_out.reshape(k_cache.shape), v_out.reshape(v_cache.shape)

    request_spec = P("dp", None, None)
    node_spec = P("dp", None)
    cache_spec = P("dp", None, "tp", None)
    shared_spec = P(None)
    column_spec = P(None, "tp")
    row_spec = P("tp", None)
    in_specs = (request_spec, request_spec, node_spec, P("dp"), node_spec, node_spec, cache_spec, cache_spec, shared_spec, column_spec, column_spec, column_spec, row_spec, shared_spec, column_spec, column_spec, row_spec, shared_spec, column_spec)
    out_specs = (node_spec, node_spec, cache_spec, cache_spec)
    return jax.shard_map(group_step, mesh=mesh, in_specs=in_specs, out_specs=out_specs, check_vma=False)
```

```python
import functools

import jax
import jax.numpy as jnp
import numpy as np
from jax import lax
from jax.experimental import pallas as pl
from jax.experimental.pallas import tpu as pltpu
from jax.sharding import PartitionSpec as P

RMS_EPS = 1e-5
ROPE_THETA = 500000
STEPS = 4
SPAN = 1024
GATE = 512
HEAD = 1024
TILE = 512
VMEM_LIMIT = 66_000_000
HBM = pl.BlockSpec(memory_space=pl.ANY)
VMEM = pl.BlockSpec(memory_space=pltpu.VMEM)
LAST = (((1,), (1,)), ((), ()))
SMEM = pl.BlockSpec(memory_space=pltpu.SMEM)


def norm_rows(wide, gain):
    scale = lax.rsqrt(jnp.mean(wide * wide, axis=-1, keepdims=True) + RMS_EPS)
    return (wide * scale * gain).astype(jnp.bfloat16)


def gain_row(ref):
    wide = ref[...].astype(jnp.float32)
    return jnp.concatenate([wide[i:i + 1, :] for i in range(wide.shape[0])], axis=1)


def window_pages(nodes, page_size):
    return -(-(nodes - 1) // page_size) + 1


def column_of(ref, b):
    nodes = ref.shape[1]
    down = lax.broadcasted_iota(jnp.int32, (nodes, nodes), 0)
    across = lax.broadcasted_iota(jnp.int32, (nodes, nodes), 1)
    row = ref[pl.ds(b, 1), :].astype(jnp.float32)
    return jnp.sum(jnp.where(down == across, row, 0.0), axis=-1, keepdims=True)


def attention_kernel(
    dims, ctx_ref, table_ref, depth_ref, freq_ref, hidden_hbm, gain_ref, mask_ref, wq_hbm, wk_hbm, wv_hbm, k_hbm, v_hbm,
    att_ref, k_out, v_out, hid, normed, weights, kc, vc, cosine, sine, gain_buf, head_bias, q_buf, k_buf, v_buf, o_buf, renewed, in_sems, out_sems,
):
    requests, nodes, pages, page_rows, heads, head_dim = dims
    rows = requests * nodes
    stack = heads * nodes
    span_rows = pages * page_rows
    half_rows = rows // 2
    f32, bf16, i32 = jnp.float32, jnp.bfloat16, jnp.int32
    copies = []
    for part in range(2):
        piece = pl.ds(part * half_rows, half_rows)
        copies.append(pltpu.make_async_copy(hidden_hbm.at[piece], hid.at[piece], in_sems.at[part]))
    for i, w in enumerate((wq_hbm, wk_hbm, wv_hbm)):
        copies.append(pltpu.make_async_copy(w, weights.at[i], in_sems.at[2 + i]))
    copies.append(pltpu.make_async_copy(k_hbm, kc, in_sems.at[5]))
    copies.append(pltpu.make_async_copy(v_hbm, vc, in_sems.at[6]))
    for copy in copies[:3]:
        copy.start()

    gain_buf[...] = gain_row(gain_ref)
    lane = lax.broadcasted_iota(i32, (1, head_dim), 1)
    sign = jnp.where(lane < head_dim // 2, -1.0, 1.0)

    def angle_step(b, _):
        mine = pl.ds(pl.multiple_of(b * nodes, 8), nodes)
        angle = (column_of(depth_ref, b) + ctx_ref[b].astype(f32)) * freq_ref[...]
        cosine[mine, :] = jnp.cos(angle)
        sine[mine, :] = jnp.sin(angle) * sign
        return 0

    lax.fori_loop(0, requests, angle_step, 0)
    for copy in copies[3:]:
        copy.start()
    span_col = lax.broadcasted_iota(i32, (1, span_rows), 1)
    slot_col = span_col // heads
    stack_row = lax.broadcasted_iota(i32, (stack, 1), 0)
    stack_col = lax.broadcasted_iota(i32, (1, stack), 1)
    head_bias[...] = jnp.where((span_col % heads) == (stack_row // nodes), 0.0, -jnp.inf)

    group = 16
    for part in range(2):
        copies[part].wait()

        def norm_step(i, _, part=part):
            gain = gain_buf[...]
            at = [pl.ds(pl.multiple_of(part * half_rows + (i * 2 + k) * group, group), group) for k in range(2)]
            scales = []
            for p in at:
                wide = hid[p, :].astype(f32)
                scales.append(lax.rsqrt(jnp.mean(wide * wide, axis=-1, keepdims=True) + RMS_EPS))
            for p, scale in zip(at, scales):
                normed[p, :] = (hid[p, :].astype(f32) * scale * gain).astype(bf16)
            return 0

        lax.fori_loop(0, half_rows // group // 2, norm_step, 0)

    flush = [pltpu.make_async_copy(cache, out, out_sems.at[k]) for k, (cache, out) in enumerate(((kc, k_out), (vc, v_out)))]
    width = heads * head_dim
    for i, buf in enumerate((q_buf, k_buf, v_buf)):
        copies[2 + i].wait()

        def project(t, _, i=i, buf=buf):
            cols = pl.ds(pl.multiple_of(t * TILE, TILE), TILE)
            out = jnp.dot(normed[...], weights[i, :, cols], preferred_element_type=f32)
            for h in range(TILE // head_dim):
                one = out[:, h * head_dim:(h + 1) * head_dim]
                if i < 2:
                    one = one * cosine[...] + pltpu.roll(one, head_dim // 2, 1) * sine[...]
                one = one.astype(bf16).astype(f32)
                at = pl.ds(pl.multiple_of(t * TILE + h * head_dim, head_dim), head_dim)
                buf[:, at] = one
            return 0

        lax.fori_loop(0, width // TILE, project, 0)
        if i == 1:
            for k, whole in enumerate(flush):
                copies[5 + k].wait()
                whole.start()

    touched = window_pages(nodes, page_rows // heads)
    window = touched * page_rows
    row_id = lax.broadcasted_iota(i32, (window, 1), 0)
    put = (stack_col % nodes) * heads + stack_col // nodes
    expand = ((stack_row % nodes) == lax.broadcasted_iota(i32, (1, nodes), 1)).astype(bf16)
    spread = ((stack_col % nodes) == lax.broadcasted_iota(i32, (nodes, 1), 0)).astype(bf16)
    same_head = (stack_row // nodes) == (stack_col // nodes)
    scale = head_dim ** -0.5

    def attend(b):
        ctx = ctx_ref[b]
        at = [pl.ds(pl.multiple_of(table_ref[b, j] * page_rows, page_rows), page_rows) for j in range(pages)]
        mine = pl.ds(pl.multiple_of(b * nodes, 8), nodes)

        def stacked(buf):
            parts = [buf[mine, h * head_dim:(h + 1) * head_dim] for h in range(heads)]
            return jnp.concatenate(parts, axis=0).astype(bf16)

        query, key, val = stacked(q_buf), stacked(k_buf), stacked(v_buf)
        keys = jnp.concatenate([kc[p, :] for p in at], axis=0)
        vals = jnp.concatenate([vc[p, :] for p in at], axis=0)
        first = jnp.minimum(ctx // (page_rows // heads), pages - touched)
        shift = ctx * heads - first * page_rows
        place = (put + shift == row_id).astype(bf16)
        fresh = (row_id >= shift) & (row_id < shift + stack)
        new = jnp.dot(place, jnp.concatenate([key, val], axis=1), preferred_element_type=f32)
        tree = mask_ref[b].astype(f32).astype(bf16)
        tree = jnp.dot(expand, tree, preferred_element_type=f32).astype(bf16)
        tree = jnp.dot(tree, spread, preferred_element_type=f32)
        score = lax.dot_general(query, keys, LAST, preferred_element_type=f32) * scale
        slot_bias = jnp.where(slot_col < ctx, 0.0, -jnp.inf)
        score = score + (head_bias[...] + slot_bias)
        score_new = lax.dot_general(query, key, LAST, preferred_element_type=f32) * scale
        score_new = jnp.where(same_head & (tree > 0.5), score_new, -jnp.inf)
        top = jnp.maximum(jnp.max(score, axis=-1, keepdims=True), jnp.max(score_new, axis=-1, keepdims=True))
        prob = jnp.exp(score - top)
        prob_new = jnp.exp(score_new - top)
        total = jnp.sum(prob, axis=-1, keepdims=True) + jnp.sum(prob_new, axis=-1, keepdims=True)
        mixed = jnp.dot(prob.astype(bf16), vals, preferred_element_type=f32)
        mixed = (mixed + jnp.dot(prob_new.astype(bf16), val, preferred_element_type=f32)) / total
        stores = []
        for j in range(touched):
            page = pl.ds(pl.multiple_of(table_ref[b, first + j] * page_rows, page_rows), page_rows)
            piece = slice(j * page_rows, (j + 1) * page_rows)
            for c, cache in enumerate((kc, vc)):
                fill = new[piece, c * head_dim:(c + 1) * head_dim]
                old = cache[page, :].astype(f32)
                stores.append((c, j, page, jnp.where(fresh[piece], fill, old).astype(bf16)))
        return mine, mixed, stores

    together = 4
    for whole in flush:
        whole.wait()

    def request_step(i, _):
        done = [attend(i * together + k) for k in range(together)]
        for k, (mine, mixed, stores) in enumerate(done):
            for h in range(heads):
                o_buf[mine, h * head_dim:(h + 1) * head_dim] = mixed[h * nodes:(h + 1) * nodes]
            for c, j, page, value in stores:
                slot = pl.ds(pl.multiple_of((i * together + k) * window + j * page_rows, page_rows), page_rows)
                renewed[c, slot, :] = value
        for k, (mine, mixed, stores) in enumerate(done):
            for c, j, page, value in stores:
                slot = pl.ds(pl.multiple_of((i * together + k) * window + j * page_rows, page_rows), page_rows)
                out = (k_out, v_out)[c]
                pltpu.make_async_copy(renewed.at[c, slot, :], out.at[page, :], out_sems.at[2 + c]).start()
        return 0

    lax.fori_loop(0, requests // together, request_step, 0)
    att_ref[...] = o_buf[...].astype(bf16)
    for c, out in enumerate((k_out, v_out)):
        pltpu.make_async_copy(renewed.at[c], out.at[pl.ds(0, requests * window), :], out_sems.at[2 + c]).wait()


def attention(hidden, tree_mask, depth, ctx_len, block_table, freq, k_pages, v_pages, attn_norm, w_q, w_k, w_v, dims):
    requests, nodes, pages, page_rows, heads, head_dim = dims
    rows = requests * nodes
    model = hidden.shape[1]
    width = heads * head_dim
    bf16, f32 = jnp.bfloat16, jnp.float32
    window = window_pages(nodes, page_rows // heads) * page_rows
    scratch = [
        pltpu.VMEM((rows, model), bf16),
        pltpu.VMEM((rows, model), bf16),
        pltpu.VMEM((3, model, width), bf16),
        pltpu.VMEM(k_pages.shape, bf16),
        pltpu.VMEM(v_pages.shape, bf16),
        pltpu.VMEM((rows, head_dim), f32),
        pltpu.VMEM((rows, head_dim), f32),
        pltpu.VMEM((1, model), f32),
        pltpu.VMEM((heads * nodes, pages * page_rows), f32),
    ] + [pltpu.VMEM((rows, width), f32)] * 4 + [pltpu.VMEM((2, requests * window, head_dim), bf16), pltpu.SemaphoreType.DMA((7,)), pltpu.SemaphoreType.DMA((4,))]
    return pl.pallas_call(
        functools.partial(attention_kernel, dims),
        name="attend",
        out_shape=(
            jax.ShapeDtypeStruct((rows, width), bf16),
            jax.ShapeDtypeStruct(k_pages.shape, bf16),
            jax.ShapeDtypeStruct(v_pages.shape, bf16),
        ),
        in_specs=[SMEM, SMEM, VMEM, VMEM, HBM, VMEM, VMEM, HBM, HBM, HBM, HBM, HBM],
        out_specs=(VMEM, HBM, HBM),
        scratch_shapes=scratch,
        compiler_params=pltpu.CompilerParams(vmem_limit_bytes=VMEM_LIMIT),
    )(ctx_len, block_table, depth, freq, hidden, attn_norm, tree_mask, w_q, w_k, w_v, k_pages, v_pages)


def tail_kernel(
    chips, att_ref, hid_hbm, mlp_gain_ref, fin_gain_ref, score_ref, wo_hbm, wg_hbm, wu_hbm, wd_hbm, lm_hbm,
    top_ref, total_ref, pick_ref, part, sib_in, rel_l, rel_r, in_l, in_r, xg, act, hid_own, run_max, run_sum, run_pick, stats, want_ref, gains,
    send_sems, recv_sems, stat_send, stat_recv, w_sems, wo_sems, lm_sems, hid_sem,
):
    f32, bf16 = jnp.float32, jnp.bfloat16
    rows, model = xg.shape
    ffn = wg_hbm.shape[0]
    vocab = lm_hbm.shape[0]
    members = 2 * chips
    size = rows // members
    quarter = size * chips
    wide = model // STEPS
    sub = wide // 2
    me = lax.axis_index("tp")
    x = me // 2
    core = me % 2
    right = lax.rem(x + 1, chips) * 2 + core
    left = lax.rem(x + chips - 1, chips) * 2 + core
    sib = x * 2 + 1 - core

    barrier = pltpu.get_barrier_semaphore()
    for k in range(1, members):
        pl.semaphore_signal(barrier, inc=1, device_id={"tp": lax.rem(me + k, members)}, device_id_type=pl.DeviceIdType.MESH)

    def first_row(hop):
        return (core * chips + lax.rem(x + hop + chips, chips)) * size

    def block(hop):
        return pl.ds(pl.multiple_of(first_row(hop), 16), size)

    def lanes_of(start, width):
        return pl.ds(start if isinstance(start, int) else pl.multiple_of(start, 128), width)

    def cols(c, part=None):
        if part is None:
            return lanes_of(c * wide, wide)
        return lanes_of(c * wide + part * sub, sub)

    def plan(phase, c, name):
        far = pl.ds(pl.multiple_of((1 - core) * quarter, 16), quarter)
        own, opp, rgt, lft = block(0), block(2), block(1), block(-1)
        both = cols(c)
        c0, c1, here = cols(c, 0), cols(c, 1), lanes_of(c * sub, sub)
        entries = [
            ("pair", part.at[far, both], sib_in.at[:, both], sib),
            ("relay_r", part.at[opp, c0], rel_l.at[:, here], right),
            ("relay_l", part.at[opp, c1], rel_r.at[:, here], left),
            ("direct_r", part.at[rgt, c1], in_l.at[:, c1], right),
            ("direct_l", part.at[lft, c0], in_r.at[:, c0], left),
            ("acc_r", part.at[rgt, c0], in_l.at[:, c0], right),
            ("acc_l", part.at[lft, c1], in_r.at[:, c1], left),
            ("own_r0", xg.at[own, c0], xg.at[own, c0], right),
            ("own_l1", xg.at[own, c1], xg.at[own, c1], left),
            ("own_r1", xg.at[own, c1], xg.at[own, c1], right),
            ("own_l0", xg.at[own, c0], xg.at[own, c0], left),
            ("own_s", xg.at[own, both], xg.at[own, both], sib),
            ("fwd_r", xg.at[lft, c0], xg.at[lft, c0], right),
            ("fwd_l", xg.at[rgt, c1], xg.at[rgt, c1], left),
            ("lft_s", xg.at[lft, both], xg.at[lft, both], sib),
            ("rgt_s", xg.at[rgt, both], xg.at[rgt, both], sib),
            ("opp_s", xg.at[opp, both], xg.at[opp, both], sib),
        ]
        i = [entry[0] for entry in entries].index(name)
        _, src, dst, to = entries[i]
        return pltpu.make_async_remote_copy(
            src_ref=src, dst_ref=dst, send_sem=send_sems.at[phase, c, i], recv_sem=recv_sems.at[phase, c, i],
            device_id={"tp": to}, device_id_type=pl.DeviceIdType.MESH,
        )

    reduce_names = ("pair", "relay_r", "relay_l", "direct_r", "direct_l", "acc_r", "acc_l")
    own_names = ("own_r0", "own_l1", "own_r1", "own_l0", "own_s")
    other_names = ("fwd_r", "fwd_l", "lft_s", "rgt_s", "opp_s")
    steps = range(STEPS)

    def pair_sum(phase, c):
        both = cols(c)
        plan(phase, c, "pair").wait_recv()

        def add(i, _):
            there = pl.ds(pl.multiple_of(core * quarter + i * 32, 16), 32)
            here = pl.ds(pl.multiple_of(i * 32, 32), 32)
            part[there, both] = (part[there, both].astype(f32) + sib_in[here, both].astype(f32)).astype(bf16)
            return 0

        lax.fori_loop(0, quarter // 32, add, 0)
        for name in ("relay_r", "relay_l", "direct_r", "direct_l"):
            plan(phase, c, name).start()

    def accumulate(phase, c):
        here = lanes_of(c * sub, sub)
        for name, hop, which, buf in (("r", 1, 0, rel_l), ("l", -1, 1, rel_r)):
            plan(phase, c, f"relay_{name}").wait_recv()
            at = block(hop)
            part[at, cols(c, which)] = (part[at, cols(c, which)].astype(f32) + buf[:, here].astype(f32)).astype(bf16)
            plan(phase, c, f"acc_{name}").start()

    def own_send(phase, c):
        for name in own_names:
            plan(phase, c, name).start()

    def finish(phase):
        squares = 0.0
        for c in steps:
            both = cols(c)
            for name in ("direct_r", "direct_l", "acc_r", "acc_l"):
                plan(phase, c, name).wait_recv()
            total = part[block(0), both].astype(f32) + in_l[:, both].astype(f32) + in_r[:, both].astype(f32)
            residual = (hid_own[:, both].astype(f32) + total.astype(bf16).astype(f32)).astype(bf16)
            hid_own[:, both] = residual
            full = residual.astype(f32)
            squares = squares + jnp.sum(full * full, axis=-1, keepdims=True)
        scale = lax.rsqrt(squares * (1.0 / model) + RMS_EPS)
        for c in steps:
            both = cols(c)
            xg[block(0), both] = (hid_own[:, both].astype(f32) * scale * gains[phase:phase + 1, both]).astype(bf16)
            if c < 2:
                own_send(phase, c)

    def forward(phase, c, more=True):
        plan(phase, c, "own_r0").wait_recv()
        plan(phase, c, "fwd_r").start()
        plan(phase, c, "own_l1").wait_recv()
        plan(phase, c, "fwd_l").start()
        if more:
            own_send(phase, c + 2)

    def share(phase, c):
        plan(phase, c, "own_r1").wait_recv()
        plan(phase, c, "lft_s").start()
        plan(phase, c, "own_l0").wait_recv()
        plan(phase, c, "rgt_s").start()
        plan(phase, c, "fwd_r").wait_recv()
        plan(phase, c, "fwd_l").wait_recv()
        plan(phase, c, "opp_s").start()

    def ready(phase, c):
        for name in ("own_s", "lft_s", "rgt_s", "opp_s"):
            plan(phase, c, name).wait_recv()

    def drain(phase):
        def one(c, _):
            for name in reduce_names + own_names + other_names:
                plan(phase, c, name).wait_send()
            return 0

        lax.fori_loop(0, STEPS, one, 0)

    def reduce_start(phase, lhs_ref, w_ref, before):
        def step(c, _):
            before(c)
            part[:, cols(c)] = jnp.dot(lhs_ref[...], w_ref[:, cols(c)], preferred_element_type=f32).astype(bf16)
            plan(phase, c, "pair").start()

            @pl.when(c >= 1)
            def _():
                pair_sum(phase, c - 1)

            @pl.when(c >= 3)
            def _():
                accumulate(phase, c - 3)

            return 0

        lax.fori_loop(0, STEPS, step, 0)

    def reduce_end(phase, filler):
        def step(c, _):
            @pl.when(c <= STEPS)
            def _():
                pair_sum(phase, c - 1)

            accumulate(phase, c - 3)
            return 0

        lax.fori_loop(STEPS, STEPS + 3, step, 0)
        filler()
        finish(phase)

    def gather(phase, compute, loads, early):
        forward(phase, 0)
        forward(phase, 1)
        share(phase, 0)
        ready(phase, 0)
        forward(phase, 2, False)
        for load in loads:
            load.wait()

        def step(c, _):
            compute(cols(c), False, 0)

            @pl.when(c <= 1)
            def _():
                share(phase, c + 1)

            @pl.when(c == 0)
            def _():
                forward(phase, 3, False)

            compute(cols(c), False, 1)

            @pl.when(c == 1)
            def _():
                share(phase, 3)

            @pl.when(c + 1 < early)
            def _():
                ready(phase, c + 1)

            return 0

        lax.fori_loop(0, early, step, 0)
        for c in range(early, STEPS):
            ready(phase, c)
        compute(pl.ds(early * wide, (STEPS - early) * wide), True, None)

    def layer(wo, wg, wu, wd, gate_acc, up_acc):
        loads = [
            pltpu.make_async_copy(src, dst, w_sems.at[i])
            for i, (src, dst) in enumerate(((wg_hbm, wg), (wu_hbm, wu), (wd_hbm, wd)))
        ]
        def wo_piece(c):
            return pltpu.make_async_copy(wo_hbm.at[:, cols(c)], wo.at[:, cols(c)], wo_sems.at[c])

        for c in steps:
            wo_piece(c).start()
        own_rows = pltpu.make_async_copy(hid_hbm.at[block(0), :], hid_own, hid_sem.at[0])
        own_rows.start()

        def before(c):
            wo_piece(c).wait()

            @pl.when(c == STEPS - 1)
            def _():
                for load in loads:
                    load.start()

        def filler():
            gains[0:1, :] = gain_row(mlp_gain_ref)
            gains[1:2, :] = gain_row(fin_gain_ref)
            gate_acc[...] = jnp.zeros(gate_acc.shape, f32)
            up_acc[...] = jnp.zeros(up_acc.shape, f32)
            own_rows.wait()

        pl.semaphore_wait(barrier, members - 1)
        reduce_start(0, att_ref, wo, before)
        reduce_end(0, filler)

        def gated(span, is_last, half):
            def close(start, width):
                at = pl.ds(start, width)
                gate = gate_acc[:, at]
                act[:, at] = (gate * jax.nn.sigmoid(gate) * up_acc[:, at]).astype(bf16)

            def tile(start, width):
                at = pl.ds(start, width)
                for w, acc in ((wg, gate_acc), (wu, up_acc)):
                    acc[:, at] += lax.dot_general(xg[:, span], w[at, span], LAST, preferred_element_type=f32)

            def step(t, _):
                tile(pl.multiple_of(t * GATE, GATE), GATE)
                return 0

            full = ffn // GATE
            if is_last:
                pieces = [(t * GATE, min(GATE, ffn - t * GATE)) for t in range(-(-ffn // GATE))]
                tile(*pieces[0])
                for t in range(1, len(pieces)):
                    close(*pieces[t - 1])
                    tile(*pieces[t])
                close(*pieces[-1])
            elif half == 0:
                lax.fori_loop(0, full, step, 0)
            else:
                tile(full * GATE, ffn - full * GATE)

        gather(0, gated, loads[:2], STEPS - 1)
        drain(0)
        loads[2].wait()
        reduce_start(1, act, wd, lambda c: None)

    pl.run_scoped(
        layer,
        pltpu.VMEM(wo_hbm.shape, bf16), pltpu.VMEM((ffn, model), bf16), pltpu.VMEM((ffn, model), bf16), pltpu.VMEM((ffn, model), bf16),
        pltpu.VMEM((rows, ffn), f32), pltpu.VMEM((rows, ffn), f32),
    )

    pieces = 5
    lanes = 128

    def head(lm, acc):
        loads = []
        step_rows = vocab // pieces
        for i in range(pieces):
            piece = pl.ds(i * step_rows, step_rows)
            loads.append(pltpu.make_async_copy(lm_hbm.at[piece, :], lm.at[piece, :], lm_sems.at[i]))
            loads[-1].start()

        def want_step(b, _):
            nodes = score_ref.shape[1]
            column = column_of(score_ref, b).astype(jnp.int32)
            want_ref[pl.ds(pl.multiple_of(b * nodes, 8), nodes), :] = jnp.broadcast_to(column, (nodes, 128))
            return 0

        run_max[...] = jnp.full(run_max.shape, -jnp.inf, f32)
        run_sum[...] = jnp.zeros(run_sum.shape, f32)
        run_pick[...] = jnp.zeros(run_pick.shape, f32)
        full = vocab // HEAD
        rest = vocab % HEAD
        whole = rest // lanes * lanes

        def fold(base, width):
            parts = [acc[:, pl.ds(base + i * lanes, lanes)] for i in range(width // lanes)]
            old = run_max[...]
            new = functools.reduce(jnp.maximum, parts, old)
            lane = lax.broadcasted_iota(jnp.int32, (1, lanes), 1) + base + me * vocab
            want = want_ref[...]
            total = run_sum[...] * jnp.exp(old - new)
            pick = run_pick[...]
            for i, one in enumerate(parts):
                total = total + jnp.exp(one - new)
                pick = pick + jnp.where(lane + i * lanes == want, one, 0.0)
            run_max[...] = new
            run_sum[...] = total
            run_pick[...] = pick

        def logits(span, is_last, half):
            def tile(base, width):
                at = pl.ds(base, width)
                acc[:, at] += lax.dot_general(xg[:, span], lm[at, span], LAST, preferred_element_type=f32)

            def step(t, _):
                tile(pl.multiple_of(t * HEAD, HEAD), HEAD)
                return 0

            cut = (full + 1) // 2
            if is_last:
                for t in range(full):
                    tile(t * HEAD, HEAD)
                    if t > 0:
                        fold((t - 1) * HEAD, HEAD)
                fold((full - 1) * HEAD, HEAD)
                tile(full * HEAD, rest)
            elif half == 0:
                lax.fori_loop(0, cut, step, 0)
            else:
                lax.fori_loop(cut, full, step, 0)
                tile(full * HEAD, rest)

        def filler():
            lax.fori_loop(0, score_ref.shape[0], want_step, 0)
            acc[...] = jnp.zeros(acc.shape, f32)

        reduce_end(1, filler)
        gather(1, logits, loads, STEPS - 2)
        fold(full * HEAD, whole)
        end = acc[:, full * HEAD + whole:vocab]
        top = jnp.maximum(jnp.max(run_max[...], axis=-1, keepdims=True), jnp.max(end, axis=-1, keepdims=True))
        total = jnp.sum(run_sum[...] * jnp.exp(run_max[...] - top), axis=-1, keepdims=True)
        total = total + jnp.sum(jnp.exp(end - top), axis=-1, keepdims=True)
        lane = lax.broadcasted_iota(jnp.int32, (1, rest - whole), 1) + (full * HEAD + whole) + me * vocab
        pick = jnp.sum(run_pick[...], axis=-1, keepdims=True)
        pick = pick + jnp.sum(jnp.where(lane == want_ref[:, 0:1], end, 0.0), axis=-1, keepdims=True)
        place = lax.broadcasted_iota(jnp.int32, (1, lanes), 1)
        packed = jnp.where(place == 0, top, jnp.where(place == 1, total, pick))
        stats[me] = packed.T[0:8, :]

    pl.run_scoped(head, pltpu.VMEM((vocab, model), bf16), pltpu.VMEM((rows, vocab), f32))

    sends = []
    for k in range(1, members):
        to = lax.rem(me + k, members)
        sends.append(pltpu.make_async_remote_copy(
            src_ref=stats.at[me], dst_ref=stats.at[me], send_sem=stat_send.at[k - 1], recv_sem=stat_recv.at[k - 1],
            device_id={"tp": to}, device_id_type=pl.DeviceIdType.MESH,
        ))
        sends[-1].start()
    drain(1)
    for copy in sends:
        copy.wait()
    every = [stats[i] for i in range(members)]
    top = functools.reduce(jnp.maximum, [e[0:1, :] for e in every])
    total = functools.reduce(jnp.add, [e[1:2, :] * jnp.exp(e[0:1, :] - top) for e in every])
    pick = functools.reduce(jnp.add, [e[2:3, :] for e in every])
    requests, nodes = score_ref.shape
    for b in range(requests):
        for ref, row in ((top_ref, top), (total_ref, total), (pick_ref, pick)):
            ref[b:b + 1, :] = row[:, b * nodes:(b + 1) * nodes]


def tail(attended, hidden, mlp_norm, final_norm, score_id, w_o, w_gate, w_up, w_down, w_lm, chips):
    rows, model = hidden.shape
    ffn = w_gate.shape[0]
    members = 2 * chips
    bf16, f32 = jnp.bfloat16, jnp.float32
    own = rows // members
    scratch = [
        pltpu.VMEM((rows, model), bf16),
        pltpu.VMEM((rows // 2, model), bf16),
        pltpu.VMEM((own, model // 2), bf16),
        pltpu.VMEM((own, model // 2), bf16),
        pltpu.VMEM((own, model), bf16),
        pltpu.VMEM((own, model), bf16),
        pltpu.VMEM((rows, model), bf16),
        pltpu.VMEM((rows, ffn), bf16),
        pltpu.VMEM((own, model), bf16),
        pltpu.VMEM((rows, 128), f32),
        pltpu.VMEM((rows, 128), f32),
        pltpu.VMEM((rows, 128), f32),
        pltpu.VMEM((members, 8, rows), f32),
        pltpu.VMEM((rows, 128), jnp.int32),
        pltpu.VMEM((2, model), f32),
        pltpu.SemaphoreType.DMA((2, STEPS, 17)),
        pltpu.SemaphoreType.DMA((2, STEPS, 17)),
        pltpu.SemaphoreType.DMA((members - 1,)),
        pltpu.SemaphoreType.DMA((members - 1,)),
        pltpu.SemaphoreType.DMA((3,)),
        pltpu.SemaphoreType.DMA((STEPS,)),
        pltpu.SemaphoreType.DMA((5,)),
        pltpu.SemaphoreType.DMA((1,)),
    ]
    return pl.pallas_call(
        functools.partial(tail_kernel, chips),
        name="tail",
        out_shape=(jax.ShapeDtypeStruct(score_id.shape, f32),) * 3,
        in_specs=[VMEM, HBM, VMEM, VMEM, VMEM, HBM, HBM, HBM, HBM, HBM],
        out_specs=(VMEM, VMEM, VMEM),
        scratch_shapes=scratch,
        compiler_params=pltpu.CompilerParams(vmem_limit_bytes=VMEM_LIMIT, collective_id=0, has_side_effects=True),
    )(attended, hidden, mlp_norm, final_norm, score_id, w_o, w_gate, w_up, w_down, w_lm)


def solution(mesh):
    chips = mesh.shape["tp"] // 2

    def group_step(hidden, tree_mask, depth, ctx_len, block_table, score_id, k_cache, v_cache, attn_norm, w_q, w_k, w_v, w_o, mlp_norm, w_gate, w_up, w_down, final_norm, w_lm):
        requests, nodes, model = hidden.shape
        blocks, page_size, heads, head_dim = k_cache.shape
        dims = (requests, nodes, block_table.shape[1], page_size * heads, heads, head_dim)
        rows = requests * nodes
        flat = hidden.reshape(rows, model)
        inv_freq = 1.0 / (ROPE_THETA ** (np.arange(head_dim // 2) * (2.0 / head_dim)))
        freq = jnp.asarray(np.concatenate([inv_freq, inv_freq])[None, :], jnp.float32)
        pages = (blocks * page_size * heads, head_dim)
        attended, k_out, v_out = attention(
            flat, tree_mask, depth, ctx_len, block_table, freq, k_cache.reshape(pages), v_cache.reshape(pages),
            attn_norm.reshape(model // 128, 128), w_q, w_k, w_v, dims,
        )
        top, total, pick = tail(
            attended, flat, mlp_norm.reshape(model // 128, 128), final_norm.reshape(model // 128, 128), score_id,
            w_o, w_gate.T, w_up.T, w_down, w_lm.T, chips,
        )
        log_norm = top + jnp.log(total)
        return log_norm, pick - log_norm, k_out.reshape(k_cache.shape), v_out.reshape(v_cache.shape)

    request_spec = P("dp", None, None)
    node_spec = P("dp", None)
    cache_spec = P("dp", None, "tp", None)
    shared_spec = P(None)
    column_spec = P(None, "tp")
    row_spec = P("tp", None)
    in_specs = (request_spec, request_spec, node_spec, P("dp"), node_spec, node_spec, cache_spec, cache_spec, shared_spec, column_spec, column_spec, column_spec, row_spec, shared_spec, column_spec, column_spec, row_spec, shared_spec, column_spec)
    out_specs = (node_spec, node_spec, cache_spec, cache_spec)
    return jax.shard_map(group_step, mesh=mesh, in_specs=in_specs, out_specs=out_specs, check_vma=False)
```

```python
import functools

import jax
import jax.numpy as jnp
import numpy as np
from jax import lax
from jax.experimental import pallas as pl
from jax.experimental.pallas import tpu as pltpu
from jax.sharding import PartitionSpec as P

RMS_EPS = 1e-5
ROPE_THETA = 500000
STEPS = 4
SPAN = 1024
GATE = 512
HEAD = 1024
TILE = 512
VMEM_LIMIT = 66_000_000
HBM = pl.BlockSpec(memory_space=pl.ANY)
VMEM = pl.BlockSpec(memory_space=pltpu.VMEM)
LAST = (((1,), (1,)), ((), ()))
SMEM = pl.BlockSpec(memory_space=pltpu.SMEM)


def norm_rows(wide, gain):
    scale = lax.rsqrt(jnp.mean(wide * wide, axis=-1, keepdims=True) + RMS_EPS)
    return (wide * scale * gain).astype(jnp.bfloat16)


def gain_row(ref):
    wide = ref[...].astype(jnp.float32)
    return jnp.concatenate([wide[i:i + 1, :] for i in range(wide.shape[0])], axis=1)


def window_pages(nodes, page_size):
    return -(-(nodes - 1) // page_size) + 1


def column_of(ref, b):
    nodes = ref.shape[1]
    down = lax.broadcasted_iota(jnp.int32, (nodes, nodes), 0)
    across = lax.broadcasted_iota(jnp.int32, (nodes, nodes), 1)
    row = ref[pl.ds(b, 1), :].astype(jnp.float32)
    return jnp.sum(jnp.where(down == across, row, 0.0), axis=-1, keepdims=True)


def attention_kernel(
    dims, ctx_ref, table_ref, depth_hbm, freq_hbm, hidden_hbm, gain_hbm, mask_hbm, wq_hbm, wk_hbm, wv_hbm, k_hbm, v_hbm,
    att_out, k_out, v_out, depth_ref, freq_ref, gain_ref, mask_ref, att_ref, hid, normed, weights, kc, vc, cosine, sine, gain_buf, head_bias, q_buf, k_buf, v_buf, o_buf, renewed, in_sems, out_sems, small_sems,
):
    requests, nodes, pages, page_rows, heads, head_dim = dims
    rows = requests * nodes
    stack = heads * nodes
    span_rows = pages * page_rows
    half_rows = rows // 2
    f32, bf16, i32 = jnp.float32, jnp.bfloat16, jnp.int32
    copies = []
    for part in range(2):
        piece = pl.ds(part * half_rows, half_rows)
        copies.append(pltpu.make_async_copy(hidden_hbm.at[piece], hid.at[piece], in_sems.at[part]))
    for i, w in enumerate((wq_hbm, wk_hbm, wv_hbm)):
        copies.append(pltpu.make_async_copy(w, weights.at[i], in_sems.at[2 + i]))
    copies.append(pltpu.make_async_copy(k_hbm, kc, in_sems.at[5]))
    copies.append(pltpu.make_async_copy(v_hbm, vc, in_sems.at[6]))
    small = [
        pltpu.make_async_copy(src, dst, small_sems.at[i])
        for i, (src, dst) in enumerate(((gain_hbm, gain_ref), (depth_hbm, depth_ref), (freq_hbm, freq_ref), (mask_hbm, mask_ref)))
    ]
    for copy in small + copies[:3]:
        copy.start()
    for copy in small:
        copy.wait()

    gain_buf[...] = gain_row(gain_ref)
    lane = lax.broadcasted_iota(i32, (1, head_dim), 1)
    sign = jnp.where(lane < head_dim // 2, -1.0, 1.0)

    together = 4

    def angle_step(i, _):
        for k in range(together):
            b = i * together + k
            mine = pl.ds(pl.multiple_of(b * nodes, 8), nodes)
            angle = (column_of(depth_ref, b) + ctx_ref[b].astype(f32)) * freq_ref[...]
            cosine[mine, :] = jnp.cos(angle)
            sine[mine, :] = jnp.sin(angle) * sign
        return 0

    lax.fori_loop(0, requests // together, angle_step, 0)
    for copy in copies[3:]:
        copy.start()
    span_col = lax.broadcasted_iota(i32, (1, span_rows), 1)
    slot_col = span_col // heads
    stack_row = lax.broadcasted_iota(i32, (stack, 1), 0)
    stack_col = lax.broadcasted_iota(i32, (1, stack), 1)
    head_bias[...] = jnp.where((span_col % heads) == (stack_row // nodes), 0.0, -jnp.inf)

    group = 16
    for part in range(2):
        copies[part].wait()

        def norm_step(i, _, part=part):
            gain = gain_buf[...]
            at = [pl.ds(pl.multiple_of(part * half_rows + (i * 2 + k) * group, group), group) for k in range(2)]
            scales = []
            for p in at:
                wide = hid[p, :].astype(f32)
                scales.append(lax.rsqrt(jnp.mean(wide * wide, axis=-1, keepdims=True) + RMS_EPS))
            for p, scale in zip(at, scales):
                normed[p, :] = (hid[p, :].astype(f32) * scale * gain).astype(bf16)
            return 0

        lax.fori_loop(0, half_rows // group // 2, norm_step, 0)

    flush = [pltpu.make_async_copy(cache, out, out_sems.at[k]) for k, (cache, out) in enumerate(((kc, k_out), (vc, v_out)))]
    width = heads * head_dim
    for i, buf in enumerate((q_buf, k_buf, v_buf)):
        copies[2 + i].wait()

        def project(t, _, i=i, buf=buf):
            cols = pl.ds(pl.multiple_of(t * TILE, TILE), TILE)
            out = jnp.dot(normed[...], weights[i, :, cols], preferred_element_type=f32)
            for h in range(TILE // head_dim):
                one = out[:, h * head_dim:(h + 1) * head_dim]
                if i < 2:
                    one = one * cosine[...] + pltpu.roll(one, head_dim // 2, 1) * sine[...]
                one = one.astype(bf16).astype(f32)
                at = pl.ds(pl.multiple_of(t * TILE + h * head_dim, head_dim), head_dim)
                buf[:, at] = one
            return 0

        lax.fori_loop(0, width // TILE, project, 0)
        if i == 1:
            for k, whole in enumerate(flush):
                copies[5 + k].wait()
                whole.start()

    touched = window_pages(nodes, page_rows // heads)
    window = touched * page_rows
    row_id = lax.broadcasted_iota(i32, (window, 1), 0)
    put = (stack_col % nodes) * heads + stack_col // nodes
    expand = ((stack_row % nodes) == lax.broadcasted_iota(i32, (1, nodes), 1)).astype(bf16)
    spread = ((stack_col % nodes) == lax.broadcasted_iota(i32, (nodes, 1), 0)).astype(bf16)
    same_head = (stack_row // nodes) == (stack_col // nodes)
    scale = head_dim ** -0.5

    def attend(b):
        ctx = ctx_ref[b]
        at = [pl.ds(pl.multiple_of(table_ref[b, j] * page_rows, page_rows), page_rows) for j in range(pages)]
        mine = pl.ds(pl.multiple_of(b * nodes, 8), nodes)

        def stacked(buf):
            parts = [buf[mine, h * head_dim:(h + 1) * head_dim] for h in range(heads)]
            return jnp.concatenate(parts, axis=0).astype(bf16)

        query, key, val = stacked(q_buf), stacked(k_buf), stacked(v_buf)
        keys = jnp.concatenate([kc[p, :] for p in at], axis=0)
        vals = jnp.concatenate([vc[p, :] for p in at], axis=0)
        first = jnp.minimum(ctx // (page_rows // heads), pages - touched)
        shift = ctx * heads - first * page_rows
        place = (put + shift == row_id).astype(bf16)
        fresh = (row_id >= shift) & (row_id < shift + stack)
        new = jnp.dot(place, jnp.concatenate([key, val], axis=1), preferred_element_type=f32)
        tree = mask_ref[b].astype(f32).astype(bf16)
        tree = jnp.dot(expand, tree, preferred_element_type=f32).astype(bf16)
        tree = jnp.dot(tree, spread, preferred_element_type=f32)
        score = lax.dot_general(query, keys, LAST, preferred_element_type=f32) * scale
        slot_bias = jnp.where(slot_col < ctx, 0.0, -jnp.inf)
        score = score + (head_bias[...] + slot_bias)
        score_new = lax.dot_general(query, key, LAST, preferred_element_type=f32) * scale
        score_new = jnp.where(same_head & (tree > 0.5), score_new, -jnp.inf)
        top = jnp.maximum(jnp.max(score, axis=-1, keepdims=True), jnp.max(score_new, axis=-1, keepdims=True))
        prob = jnp.exp(score - top)
        prob_new = jnp.exp(score_new - top)
        total = jnp.sum(prob, axis=-1, keepdims=True) + jnp.sum(prob_new, axis=-1, keepdims=True)
        mixed = jnp.dot(prob.astype(bf16), vals, preferred_element_type=f32)
        mixed = (mixed + jnp.dot(prob_new.astype(bf16), val, preferred_element_type=f32)) / total
        stores = []
        for j in range(touched):
            page = pl.ds(pl.multiple_of(table_ref[b, first + j] * page_rows, page_rows), page_rows)
            piece = slice(j * page_rows, (j + 1) * page_rows)
            for c, cache in enumerate((kc, vc)):
                fill = new[piece, c * head_dim:(c + 1) * head_dim]
                old = cache[page, :].astype(f32)
                stores.append((c, j, page, jnp.where(fresh[piece], fill, old).astype(bf16)))
        return mine, mixed, stores

    for whole in flush:
        whole.wait()

    def request_step(i, _):
        done = [attend(i * together + k) for k in range(together)]
        for k, (mine, mixed, stores) in enumerate(done):
            for h in range(heads):
                o_buf[mine, h * head_dim:(h + 1) * head_dim] = mixed[h * nodes:(h + 1) * nodes]
            for c, j, page, value in stores:
                slot = pl.ds(pl.multiple_of((i * together + k) * window + j * page_rows, page_rows), page_rows)
                renewed[c, slot, :] = value
        for k, (mine, mixed, stores) in enumerate(done):
            for c, j, page, value in stores:
                slot = pl.ds(pl.multiple_of((i * together + k) * window + j * page_rows, page_rows), page_rows)
                out = (k_out, v_out)[c]
                pltpu.make_async_copy(renewed.at[c, slot, :], out.at[page, :], out_sems.at[2 + c]).start()
        return 0

    lax.fori_loop(0, requests // together, request_step, 0)
    att_ref[...] = o_buf[...].astype(bf16)
    att_copy = pltpu.make_async_copy(att_ref, att_out, small_sems.at[4])
    att_copy.start()
    for c, out in enumerate((k_out, v_out)):
        pltpu.make_async_copy(renewed.at[c], out.at[pl.ds(0, requests * window), :], out_sems.at[2 + c]).wait()
    att_copy.wait()


def attention(hidden, tree_mask, depth, ctx_len, block_table, freq, k_pages, v_pages, attn_norm, w_q, w_k, w_v, dims):
    requests, nodes, pages, page_rows, heads, head_dim = dims
    rows = requests * nodes
    model = hidden.shape[1]
    width = heads * head_dim
    bf16, f32 = jnp.bfloat16, jnp.float32
    window = window_pages(nodes, page_rows // heads) * page_rows
    scratch = [
        pltpu.VMEM(depth.shape, jnp.int32),
        pltpu.VMEM(freq.shape, f32),
        pltpu.VMEM(attn_norm.shape, bf16),
        pltpu.VMEM(tree_mask.shape, jnp.int32),
        pltpu.VMEM((rows, width), bf16),
        pltpu.VMEM((rows, model), bf16),
        pltpu.VMEM((rows, model), bf16),
        pltpu.VMEM((3, model, width), bf16),
        pltpu.VMEM(k_pages.shape, bf16),
        pltpu.VMEM(v_pages.shape, bf16),
        pltpu.VMEM((rows, head_dim), f32),
        pltpu.VMEM((rows, head_dim), f32),
        pltpu.VMEM((1, model), f32),
        pltpu.VMEM((heads * nodes, pages * page_rows), f32),
    ] + [pltpu.VMEM((rows, width), f32)] * 4 + [pltpu.VMEM((2, requests * window, head_dim), bf16), pltpu.SemaphoreType.DMA((7,)), pltpu.SemaphoreType.DMA((4,)), pltpu.SemaphoreType.DMA((5,))]
    return pl.pallas_call(
        functools.partial(attention_kernel, dims),
        name="attend",
        out_shape=(
            jax.ShapeDtypeStruct((rows, width), bf16),
            jax.ShapeDtypeStruct(k_pages.shape, bf16),
            jax.ShapeDtypeStruct(v_pages.shape, bf16),
        ),
        in_specs=[SMEM, SMEM] + [HBM] * 10,
        out_specs=(HBM, HBM, HBM),
        scratch_shapes=scratch,
        compiler_params=pltpu.CompilerParams(vmem_limit_bytes=VMEM_LIMIT),
    )(ctx_len, block_table, depth, freq, hidden, attn_norm, tree_mask, w_q, w_k, w_v, k_pages, v_pages)


def tail_kernel(
    chips, att_hbm, hid_hbm, mlp_gain_hbm, fin_gain_hbm, score_hbm, wo_hbm, wg_hbm, wu_hbm, wd_hbm, lm_hbm,
    top_ref, total_ref, pick_ref, att_ref, mlp_gain_ref, fin_gain_ref, score_ref, part, sib_in, rel_l, rel_r, in_l, in_r, xg, act, hid_own, run_max, run_sum, run_pick, stats, want_ref, gains,
    send_sems, recv_sems, stat_send, stat_recv, w_sems, wo_sems, lm_sems, hid_sem, small_sems,
):
    f32, bf16 = jnp.float32, jnp.bfloat16
    rows, model = xg.shape
    ffn = wg_hbm.shape[0]
    vocab = lm_hbm.shape[0]
    members = 2 * chips
    size = rows // members
    quarter = size * chips
    wide = model // STEPS
    sub = wide // 2
    me = lax.axis_index("tp")
    x = me // 2
    core = me % 2
    right = lax.rem(x + 1, chips) * 2 + core
    left = lax.rem(x + chips - 1, chips) * 2 + core
    sib = x * 2 + 1 - core

    barrier = pltpu.get_barrier_semaphore()
    for k in range(1, members):
        pl.semaphore_signal(barrier, inc=1, device_id={"tp": lax.rem(me + k, members)}, device_id_type=pl.DeviceIdType.MESH)

    def first_row(hop):
        return (core * chips + lax.rem(x + hop + chips, chips)) * size

    def block(hop):
        return pl.ds(pl.multiple_of(first_row(hop), 16), size)

    def lanes_of(start, width):
        return pl.ds(start if isinstance(start, int) else pl.multiple_of(start, 128), width)

    def cols(c, part=None):
        if part is None:
            return lanes_of(c * wide, wide)
        return lanes_of(c * wide + part * sub, sub)

    def plan(phase, c, name):
        far = pl.ds(pl.multiple_of((1 - core) * quarter, 16), quarter)
        own, opp, rgt, lft = block(0), block(2), block(1), block(-1)
        both = cols(c)
        c0, c1, here = cols(c, 0), cols(c, 1), lanes_of(c * sub, sub)
        entries = [
            ("pair", part.at[far, both], sib_in.at[:, both], sib),
            ("relay_r", part.at[opp, c0], rel_l.at[:, here], right),
            ("relay_l", part.at[opp, c1], rel_r.at[:, here], left),
            ("direct_r", part.at[rgt, c1], in_l.at[:, c1], right),
            ("direct_l", part.at[lft, c0], in_r.at[:, c0], left),
            ("acc_r", part.at[rgt, c0], in_l.at[:, c0], right),
            ("acc_l", part.at[lft, c1], in_r.at[:, c1], left),
            ("own_r0", xg.at[own, c0], xg.at[own, c0], right),
            ("own_l1", xg.at[own, c1], xg.at[own, c1], left),
            ("own_r1", xg.at[own, c1], xg.at[own, c1], right),
            ("own_l0", xg.at[own, c0], xg.at[own, c0], left),
            ("own_s", xg.at[own, both], xg.at[own, both], sib),
            ("fwd_r", xg.at[lft, c0], xg.at[lft, c0], right),
            ("fwd_l", xg.at[rgt, c1], xg.at[rgt, c1], left),
            ("lft_s", xg.at[lft, both], xg.at[lft, both], sib),
            ("rgt_s", xg.at[rgt, both], xg.at[rgt, both], sib),
            ("opp_s", xg.at[opp, both], xg.at[opp, both], sib),
        ]
        i = [entry[0] for entry in entries].index(name)
        _, src, dst, to = entries[i]
        return pltpu.make_async_remote_copy(
            src_ref=src, dst_ref=dst, send_sem=send_sems.at[phase, c, i], recv_sem=recv_sems.at[phase, c, i],
            device_id={"tp": to}, device_id_type=pl.DeviceIdType.MESH,
        )

    reduce_names = ("pair", "relay_r", "relay_l", "direct_r", "direct_l", "acc_r", "acc_l")
    own_names = ("own_r0", "own_l1", "own_r1", "own_l0", "own_s")
    other_names = ("fwd_r", "fwd_l", "lft_s", "rgt_s", "opp_s")
    steps = range(STEPS)

    def pair_sum(phase, c):
        both = cols(c)
        plan(phase, c, "pair").wait_recv()

        def add(i, _):
            there = pl.ds(pl.multiple_of(core * quarter + i * 32, 16), 32)
            here = pl.ds(pl.multiple_of(i * 32, 32), 32)
            part[there, both] = (part[there, both].astype(f32) + sib_in[here, both].astype(f32)).astype(bf16)
            return 0

        lax.fori_loop(0, quarter // 32, add, 0)
        for name in ("relay_r", "relay_l", "direct_r", "direct_l"):
            plan(phase, c, name).start()

    def accumulate(phase, c):
        here = lanes_of(c * sub, sub)
        for name, hop, which, buf in (("r", 1, 0, rel_l), ("l", -1, 1, rel_r)):
            plan(phase, c, f"relay_{name}").wait_recv()
            at = block(hop)
            part[at, cols(c, which)] = (part[at, cols(c, which)].astype(f32) + buf[:, here].astype(f32)).astype(bf16)
            plan(phase, c, f"acc_{name}").start()

    def own_send(phase, c):
        for name in own_names:
            plan(phase, c, name).start()

    def finish(phase):
        squares = 0.0
        for c in steps:
            both = cols(c)
            for name in ("direct_r", "direct_l", "acc_r", "acc_l"):
                plan(phase, c, name).wait_recv()
            total = part[block(0), both].astype(f32) + in_l[:, both].astype(f32) + in_r[:, both].astype(f32)
            residual = (hid_own[:, both].astype(f32) + total.astype(bf16).astype(f32)).astype(bf16)
            hid_own[:, both] = residual
            full = residual.astype(f32)
            squares = squares + jnp.sum(full * full, axis=-1, keepdims=True)
        scale = lax.rsqrt(squares * (1.0 / model) + RMS_EPS)
        for c in steps:
            both = cols(c)
            xg[block(0), both] = (hid_own[:, both].astype(f32) * scale * gains[phase:phase + 1, both]).astype(bf16)
            if c < 2:
                own_send(phase, c)

    def forward(phase, c, more=True):
        plan(phase, c, "own_r0").wait_recv()
        plan(phase, c, "fwd_r").start()
        plan(phase, c, "own_l1").wait_recv()
        plan(phase, c, "fwd_l").start()
        if more:
            own_send(phase, c + 2)

    def share(phase, c):
        plan(phase, c, "own_r1").wait_recv()
        plan(phase, c, "lft_s").start()
        plan(phase, c, "own_l0").wait_recv()
        plan(phase, c, "rgt_s").start()
        plan(phase, c, "fwd_r").wait_recv()
        plan(phase, c, "fwd_l").wait_recv()
        plan(phase, c, "opp_s").start()

    def ready(phase, c):
        for name in ("own_s", "lft_s", "rgt_s", "opp_s"):
            plan(phase, c, name).wait_recv()

    def drain(phase):
        def one(c, _):
            for name in reduce_names + own_names + other_names:
                plan(phase, c, name).wait_send()
            return 0

        lax.fori_loop(0, STEPS, one, 0)

    def reduce_start(phase, lhs_ref, w_ref, before):
        def step(c, _):
            before(c)
            part[:, cols(c)] = jnp.dot(lhs_ref[...], w_ref[:, cols(c)], preferred_element_type=f32).astype(bf16)
            plan(phase, c, "pair").start()

            @pl.when(c >= 1)
            def _():
                pair_sum(phase, c - 1)

            @pl.when(c >= 3)
            def _():
                accumulate(phase, c - 3)

            return 0

        lax.fori_loop(0, STEPS, step, 0)

    def reduce_end(phase, filler):
        def step(c, _):
            @pl.when(c <= STEPS)
            def _():
                pair_sum(phase, c - 1)

            accumulate(phase, c - 3)
            return 0

        lax.fori_loop(STEPS, STEPS + 3, step, 0)
        filler()
        finish(phase)

    def gather(phase, compute, loads, early):
        forward(phase, 0)
        forward(phase, 1)
        share(phase, 0)
        ready(phase, 0)
        forward(phase, 2, False)
        for load in loads:
            load.wait()

        def step(c, _):
            compute(cols(c), False, 0)

            @pl.when(c <= 1)
            def _():
                share(phase, c + 1)

            @pl.when(c == 0)
            def _():
                forward(phase, 3, False)

            compute(cols(c), False, 1)

            @pl.when(c == 1)
            def _():
                share(phase, 3)

            @pl.when(c + 1 < early)
            def _():
                ready(phase, c + 1)

            return 0

        lax.fori_loop(0, early, step, 0)
        for c in range(early, STEPS):
            ready(phase, c)
        compute(pl.ds(early * wide, (STEPS - early) * wide), True, None)

    def layer(wo, wg, wu, wd, gate_acc, up_acc):
        loads = [
            pltpu.make_async_copy(src, dst, w_sems.at[i])
            for i, (src, dst) in enumerate(((wg_hbm, wg), (wu_hbm, wu), (wd_hbm, wd)))
        ]
        def wo_piece(c):
            return pltpu.make_async_copy(wo_hbm.at[:, cols(c)], wo.at[:, cols(c)], wo_sems.at[c])

        small = [
            pltpu.make_async_copy(src, dst, small_sems.at[i])
            for i, (src, dst) in enumerate((
                (att_hbm, att_ref), (mlp_gain_hbm, mlp_gain_ref), (fin_gain_hbm, fin_gain_ref), (score_hbm, score_ref),
            ))
        ]
        small[0].start()
        for c in steps:
            wo_piece(c).start()
        for copy in small[1:]:
            copy.start()
        own_rows = pltpu.make_async_copy(hid_hbm.at[block(0), :], hid_own, hid_sem.at[0])
        own_rows.start()

        def before(c):
            wo_piece(c).wait()

            @pl.when(c == STEPS - 1)
            def _():
                for load in loads:
                    load.start()

        def filler():
            for copy in small[1:]:
                copy.wait()
            gains[0:1, :] = gain_row(mlp_gain_ref)
            gains[1:2, :] = gain_row(fin_gain_ref)
            gate_acc[...] = jnp.zeros(gate_acc.shape, f32)
            up_acc[...] = jnp.zeros(up_acc.shape, f32)
            own_rows.wait()

        small[0].wait()
        pl.semaphore_wait(barrier, members - 1)
        reduce_start(0, att_ref, wo, before)
        reduce_end(0, filler)

        def gated(span, is_last, half):
            def close(start, width):
                at = pl.ds(start, width)
                gate = gate_acc[:, at]
                act[:, at] = (gate * jax.nn.sigmoid(gate) * up_acc[:, at]).astype(bf16)

            def tile(start, width):
                at = pl.ds(start, width)
                for w, acc in ((wg, gate_acc), (wu, up_acc)):
                    acc[:, at] += lax.dot_general(xg[:, span], w[at, span], LAST, preferred_element_type=f32)

            def step(t, _):
                tile(pl.multiple_of(t * GATE, GATE), GATE)
                return 0

            full = ffn // GATE
            if is_last:
                pieces = [(t * GATE, min(GATE, ffn - t * GATE)) for t in range(-(-ffn // GATE))]
                tile(*pieces[0])
                for t in range(1, len(pieces)):
                    close(*pieces[t - 1])
                    tile(*pieces[t])
                close(*pieces[-1])
            elif half == 0:
                lax.fori_loop(0, full, step, 0)
            else:
                tile(full * GATE, ffn - full * GATE)

        gather(0, gated, loads[:2], STEPS - 1)
        drain(0)
        loads[2].wait()
        reduce_start(1, act, wd, lambda c: None)

    pl.run_scoped(
        layer,
        pltpu.VMEM(wo_hbm.shape, bf16), pltpu.VMEM((ffn, model), bf16), pltpu.VMEM((ffn, model), bf16), pltpu.VMEM((ffn, model), bf16),
        pltpu.VMEM((rows, ffn), f32), pltpu.VMEM((rows, ffn), f32),
    )

    pieces = 5
    lanes = 128

    def head(lm, acc):
        loads = []
        step_rows = vocab // pieces
        for i in range(pieces):
            piece = pl.ds(i * step_rows, step_rows)
            loads.append(pltpu.make_async_copy(lm_hbm.at[piece, :], lm.at[piece, :], lm_sems.at[i]))
            loads[-1].start()

        def want_step(b, _):
            nodes = score_ref.shape[1]
            column = column_of(score_ref, b).astype(jnp.int32)
            want_ref[pl.ds(pl.multiple_of(b * nodes, 8), nodes), :] = jnp.broadcast_to(column, (nodes, 128))
            return 0

        run_max[...] = jnp.full(run_max.shape, -jnp.inf, f32)
        run_sum[...] = jnp.zeros(run_sum.shape, f32)
        run_pick[...] = jnp.zeros(run_pick.shape, f32)
        full = vocab // HEAD
        rest = vocab % HEAD
        whole = rest // lanes * lanes

        def fold(base, width):
            parts = [acc[:, pl.ds(base + i * lanes, lanes)] for i in range(width // lanes)]
            old = run_max[...]
            new = functools.reduce(jnp.maximum, parts, old)
            lane = lax.broadcasted_iota(jnp.int32, (1, lanes), 1) + base + me * vocab
            want = want_ref[...]
            total = run_sum[...] * jnp.exp(old - new)
            pick = run_pick[...]
            for i, one in enumerate(parts):
                total = total + jnp.exp(one - new)
                pick = pick + jnp.where(lane + i * lanes == want, one, 0.0)
            run_max[...] = new
            run_sum[...] = total
            run_pick[...] = pick

        def logits(span, is_last, half):
            def tile(base, width):
                at = pl.ds(base, width)
                acc[:, at] += lax.dot_general(xg[:, span], lm[at, span], LAST, preferred_element_type=f32)

            def step(t, _):
                tile(pl.multiple_of(t * HEAD, HEAD), HEAD)
                return 0

            cut = (full + 1) // 2
            if is_last:
                for t in range(full):
                    tile(t * HEAD, HEAD)
                    if t > 0:
                        fold((t - 1) * HEAD, HEAD)
                fold((full - 1) * HEAD, HEAD)
                tile(full * HEAD, rest)
            elif half == 0:
                lax.fori_loop(0, cut, step, 0)
            else:
                lax.fori_loop(cut, full, step, 0)
                tile(full * HEAD, rest)

        def filler():
            lax.fori_loop(0, score_ref.shape[0], want_step, 0)
            acc[...] = jnp.zeros(acc.shape, f32)

        reduce_end(1, filler)
        gather(1, logits, loads, STEPS - 2)
        fold(full * HEAD, whole)
        end = acc[:, full * HEAD + whole:vocab]
        top = jnp.maximum(jnp.max(run_max[...], axis=-1, keepdims=True), jnp.max(end, axis=-1, keepdims=True))
        total = jnp.sum(run_sum[...] * jnp.exp(run_max[...] - top), axis=-1, keepdims=True)
        total = total + jnp.sum(jnp.exp(end - top), axis=-1, keepdims=True)
        lane = lax.broadcasted_iota(jnp.int32, (1, rest - whole), 1) + (full * HEAD + whole) + me * vocab
        pick = jnp.sum(run_pick[...], axis=-1, keepdims=True)
        pick = pick + jnp.sum(jnp.where(lane == want_ref[:, 0:1], end, 0.0), axis=-1, keepdims=True)
        place = lax.broadcasted_iota(jnp.int32, (1, lanes), 1)
        packed = jnp.where(place == 0, top, jnp.where(place == 1, total, pick))
        stats[me] = packed.T[0:8, :]

    pl.run_scoped(head, pltpu.VMEM((vocab, model), bf16), pltpu.VMEM((rows, vocab), f32))

    sends = []
    for k in range(1, members):
        to = lax.rem(me + k, members)
        sends.append(pltpu.make_async_remote_copy(
            src_ref=stats.at[me], dst_ref=stats.at[me], send_sem=stat_send.at[k - 1], recv_sem=stat_recv.at[k - 1],
            device_id={"tp": to}, device_id_type=pl.DeviceIdType.MESH,
        ))
        sends[-1].start()
    drain(1)
    for copy in sends:
        copy.wait()
    every = [stats[i] for i in range(members)]
    top = functools.reduce(jnp.maximum, [e[0:1, :] for e in every])
    total = functools.reduce(jnp.add, [e[1:2, :] * jnp.exp(e[0:1, :] - top) for e in every])
    pick = functools.reduce(jnp.add, [e[2:3, :] for e in every])
    requests, nodes = score_ref.shape
    for b in range(requests):
        for ref, row in ((top_ref, top), (total_ref, total), (pick_ref, pick)):
            ref[b:b + 1, :] = row[:, b * nodes:(b + 1) * nodes]


def tail(attended, hidden, mlp_norm, final_norm, score_id, w_o, w_gate, w_up, w_down, w_lm, chips):
    rows, model = hidden.shape
    ffn = w_gate.shape[0]
    members = 2 * chips
    bf16, f32 = jnp.bfloat16, jnp.float32
    own = rows // members
    scratch = [
        pltpu.VMEM(attended.shape, bf16),
        pltpu.VMEM(mlp_norm.shape, bf16),
        pltpu.VMEM(final_norm.shape, bf16),
        pltpu.VMEM(score_id.shape, jnp.int32),
        pltpu.VMEM((rows, model), bf16),
        pltpu.VMEM((rows // 2, model), bf16),
        pltpu.VMEM((own, model // 2), bf16),
        pltpu.VMEM((own, model // 2), bf16),
        pltpu.VMEM((own, model), bf16),
        pltpu.VMEM((own, model), bf16),
        pltpu.VMEM((rows, model), bf16),
        pltpu.VMEM((rows, ffn), bf16),
        pltpu.VMEM((own, model), bf16),
        pltpu.VMEM((rows, 128), f32),
        pltpu.VMEM((rows, 128), f32),
        pltpu.VMEM((rows, 128), f32),
        pltpu.VMEM((members, 8, rows), f32),
        pltpu.VMEM((rows, 128), jnp.int32),
        pltpu.VMEM((2, model), f32),
        pltpu.SemaphoreType.DMA((2, STEPS, 17)),
        pltpu.SemaphoreType.DMA((2, STEPS, 17)),
        pltpu.SemaphoreType.DMA((members - 1,)),
        pltpu.SemaphoreType.DMA((members - 1,)),
        pltpu.SemaphoreType.DMA((3,)),
        pltpu.SemaphoreType.DMA((STEPS,)),
        pltpu.SemaphoreType.DMA((5,)),
        pltpu.SemaphoreType.DMA((1,)),
        pltpu.SemaphoreType.DMA((4,)),
    ]
    return pl.pallas_call(
        functools.partial(tail_kernel, chips),
        name="tail",
        out_shape=(jax.ShapeDtypeStruct(score_id.shape, f32),) * 3,
        in_specs=[HBM] * 10,
        out_specs=(VMEM, VMEM, VMEM),
        scratch_shapes=scratch,
        compiler_params=pltpu.CompilerParams(vmem_limit_bytes=VMEM_LIMIT, collective_id=0, has_side_effects=True),
    )(attended, hidden, mlp_norm, final_norm, score_id, w_o, w_gate, w_up, w_down, w_lm)


def solution(mesh):
    chips = mesh.shape["tp"] // 2

    def group_step(hidden, tree_mask, depth, ctx_len, block_table, score_id, k_cache, v_cache, attn_norm, w_q, w_k, w_v, w_o, mlp_norm, w_gate, w_up, w_down, final_norm, w_lm):
        requests, nodes, model = hidden.shape
        blocks, page_size, heads, head_dim = k_cache.shape
        dims = (requests, nodes, block_table.shape[1], page_size * heads, heads, head_dim)
        rows = requests * nodes
        flat = hidden.reshape(rows, model)
        inv_freq = 1.0 / (ROPE_THETA ** (np.arange(head_dim // 2) * (2.0 / head_dim)))
        freq = jnp.asarray(np.concatenate([inv_freq, inv_freq])[None, :], jnp.float32)
        pages = (blocks * page_size * heads, head_dim)
        attended, k_out, v_out = attention(
            flat, tree_mask, depth, ctx_len, block_table, freq, k_cache.reshape(pages), v_cache.reshape(pages),
            attn_norm.reshape(model // 128, 128), w_q, w_k, w_v, dims,
        )
        top, total, pick = tail(
            attended, flat, mlp_norm.reshape(model // 128, 128), final_norm.reshape(model // 128, 128), score_id,
            w_o, w_gate.T, w_up.T, w_down, w_lm.T, chips,
        )
        log_norm = top + jnp.log(total)
        return log_norm, pick - log_norm, k_out.reshape(k_cache.shape), v_out.reshape(v_cache.shape)

    request_spec = P("dp", None, None)
    node_spec = P("dp", None)
    cache_spec = P("dp", None, "tp", None)
    shared_spec = P(None)
    column_spec = P(None, "tp")
    row_spec = P("tp", None)
    in_specs = (request_spec, request_spec, node_spec, P("dp"), node_spec, node_spec, cache_spec, cache_spec, shared_spec, column_spec, column_spec, column_spec, row_spec, shared_spec, column_spec, column_spec, row_spec, shared_spec, column_spec)
    out_specs = (node_spec, node_spec, cache_spec, cache_spec)
    return jax.shard_map(group_step, mesh=mesh, in_specs=in_specs, out_specs=out_specs, check_vma=False)
```

```python
import functools

import jax
import jax.numpy as jnp
import numpy as np
from jax import lax
from jax.experimental import pallas as pl
from jax.experimental.pallas import tpu as pltpu
from jax.sharding import PartitionSpec as P

RMS_EPS = 1e-5
ROPE_THETA = 500000
STEPS = 4
SPAN = 1024
GATE = 512
HEAD = 1024
TILE = 512
VMEM_LIMIT = 66_000_000
HBM = pl.BlockSpec(memory_space=pl.ANY)
VMEM = pl.BlockSpec(memory_space=pltpu.VMEM)
LAST = (((1,), (1,)), ((), ()))
SMEM = pl.BlockSpec(memory_space=pltpu.SMEM)


def norm_rows(wide, gain):
    scale = lax.rsqrt(jnp.mean(wide * wide, axis=-1, keepdims=True) + RMS_EPS)
    return (wide * scale * gain).astype(jnp.bfloat16)


def gain_row(ref):
    wide = ref[...].astype(jnp.float32)
    return jnp.concatenate([wide[i:i + 1, :] for i in range(wide.shape[0])], axis=1)


def window_pages(nodes, page_size):
    return -(-(nodes - 1) // page_size) + 1


def column_of(ref, b):
    nodes = ref.shape[1]
    down = lax.broadcasted_iota(jnp.int32, (nodes, nodes), 0)
    across = lax.broadcasted_iota(jnp.int32, (nodes, nodes), 1)
    row = ref[pl.ds(b, 1), :].astype(jnp.float32)
    return jnp.sum(jnp.where(down == across, row, 0.0), axis=-1, keepdims=True)


def attention_kernel(
    dims, ctx_ref, table_ref, depth_hbm, freq_hbm, hidden_hbm, gain_hbm, mask_hbm, wq_hbm, wk_hbm, wv_hbm, k_hbm, v_hbm,
    att_out, k_out, v_out, depth_ref, freq_ref, gain_ref, mask_ref, att_ref, hid, normed, weights, kc, vc, cosine, sine, gain_buf, head_bias, q_buf, k_buf, v_buf, o_buf, renewed, in_sems, out_sems, small_sems,
):
    requests, nodes, pages, page_rows, heads, head_dim = dims
    rows = requests * nodes
    stack = heads * nodes
    span_rows = pages * page_rows
    half_rows = rows // 2
    f32, bf16, i32 = jnp.float32, jnp.bfloat16, jnp.int32
    copies = []
    for part in range(2):
        piece = pl.ds(part * half_rows, half_rows)
        copies.append(pltpu.make_async_copy(hidden_hbm.at[piece], hid.at[piece], in_sems.at[part]))
    for i, w in enumerate((wq_hbm, wk_hbm, wv_hbm)):
        copies.append(pltpu.make_async_copy(w, weights.at[i], in_sems.at[2 + i]))
    copies.append(pltpu.make_async_copy(k_hbm, kc, in_sems.at[5]))
    copies.append(pltpu.make_async_copy(v_hbm, vc, in_sems.at[6]))
    small = [
        pltpu.make_async_copy(src, dst, small_sems.at[i])
        for i, (src, dst) in enumerate(((gain_hbm, gain_ref), (depth_hbm, depth_ref), (freq_hbm, freq_ref), (mask_hbm, mask_ref)))
    ]
    for copy in small + copies[:2]:
        copy.start()
    for copy in small:
        copy.wait()
    copies[2].start()

    gain_buf[...] = gain_row(gain_ref)
    lane = lax.broadcasted_iota(i32, (1, head_dim), 1)
    sign = jnp.where(lane < head_dim // 2, -1.0, 1.0)

    together = 4

    def angle_step(i, _):
        for k in range(together):
            b = i * together + k
            mine = pl.ds(pl.multiple_of(b * nodes, 8), nodes)
            angle = (column_of(depth_ref, b) + ctx_ref[b].astype(f32)) * freq_ref[...]
            cosine[mine, :] = jnp.cos(angle)
            sine[mine, :] = jnp.sin(angle) * sign
        return 0

    lax.fori_loop(0, requests // together, angle_step, 0)
    span_col = lax.broadcasted_iota(i32, (1, span_rows), 1)
    slot_col = span_col // heads
    stack_row = lax.broadcasted_iota(i32, (stack, 1), 0)
    stack_col = lax.broadcasted_iota(i32, (1, stack), 1)
    head_bias[...] = jnp.where((span_col % heads) == (stack_row // nodes), 0.0, -jnp.inf)

    group = 16
    for part in range(2):
        copies[part].wait()

        def norm_step(i, _, part=part):
            gain = gain_buf[...]
            at = [pl.ds(pl.multiple_of(part * half_rows + (i * 2 + k) * group, group), group) for k in range(2)]
            scales = []
            for p in at:
                wide = hid[p, :].astype(f32)
                scales.append(lax.rsqrt(jnp.mean(wide * wide, axis=-1, keepdims=True) + RMS_EPS))
            for p, scale in zip(at, scales):
                normed[p, :] = (hid[p, :].astype(f32) * scale * gain).astype(bf16)
            return 0

        lax.fori_loop(0, half_rows // group // 2, norm_step, 0)
        copies[3 + part].start()

    flush = [pltpu.make_async_copy(cache, out, out_sems.at[k]) for k, (cache, out) in enumerate(((kc, k_out), (vc, v_out)))]
    width = heads * head_dim
    for i, buf in enumerate((q_buf, k_buf, v_buf)):
        copies[2 + i].wait()

        def project(t, _, i=i, buf=buf):
            cols = pl.ds(pl.multiple_of(t * TILE, TILE), TILE)
            out = jnp.dot(normed[...], weights[i, :, cols], preferred_element_type=f32)
            for h in range(TILE // head_dim):
                one = out[:, h * head_dim:(h + 1) * head_dim]
                if i < 2:
                    one = one * cosine[...] + pltpu.roll(one, head_dim // 2, 1) * sine[...]
                one = one.astype(bf16).astype(f32)
                at = pl.ds(pl.multiple_of(t * TILE + h * head_dim, head_dim), head_dim)
                buf[:, at] = one
            return 0

        lax.fori_loop(0, width // TILE, project, 0)
        if i == 0:
            copies[5].start()
            copies[6].start()
    for k, whole in enumerate(flush):
        copies[5 + k].wait()
        whole.start()

    touched = window_pages(nodes, page_rows // heads)
    window = touched * page_rows
    row_id = lax.broadcasted_iota(i32, (window, 1), 0)
    put = (stack_col % nodes) * heads + stack_col // nodes
    expand = ((stack_row % nodes) == lax.broadcasted_iota(i32, (1, nodes), 1)).astype(bf16)
    spread = ((stack_col % nodes) == lax.broadcasted_iota(i32, (nodes, 1), 0)).astype(bf16)
    same_head = (stack_row // nodes) == (stack_col // nodes)
    scale = head_dim ** -0.5

    def attend(b):
        ctx = ctx_ref[b]
        at = [pl.ds(pl.multiple_of(table_ref[b, j] * page_rows, page_rows), page_rows) for j in range(pages)]
        mine = pl.ds(pl.multiple_of(b * nodes, 8), nodes)

        def stacked(buf):
            parts = [buf[mine, h * head_dim:(h + 1) * head_dim] for h in range(heads)]
            return jnp.concatenate(parts, axis=0).astype(bf16)

        query, key, val = stacked(q_buf), stacked(k_buf), stacked(v_buf)
        keys = jnp.concatenate([kc[p, :] for p in at], axis=0)
        vals = jnp.concatenate([vc[p, :] for p in at], axis=0)
        first = jnp.minimum(ctx // (page_rows // heads), pages - touched)
        shift = ctx * heads - first * page_rows
        place = (put + shift == row_id).astype(bf16)
        fresh = (row_id >= shift) & (row_id < shift + stack)
        new = jnp.dot(place, jnp.concatenate([key, val], axis=1), preferred_element_type=f32)
        tree = mask_ref[b].astype(f32).astype(bf16)
        tree = jnp.dot(expand, tree, preferred_element_type=f32).astype(bf16)
        tree = jnp.dot(tree, spread, preferred_element_type=f32)
        score = lax.dot_general(query, keys, LAST, preferred_element_type=f32) * scale
        slot_bias = jnp.where(slot_col < ctx, 0.0, -jnp.inf)
        score = score + (head_bias[...] + slot_bias)
        score_new = lax.dot_general(query, key, LAST, preferred_element_type=f32) * scale
        score_new = jnp.where(same_head & (tree > 0.5), score_new, -jnp.inf)
        top = jnp.maximum(jnp.max(score, axis=-1, keepdims=True), jnp.max(score_new, axis=-1, keepdims=True))
        prob = jnp.exp(score - top)
        prob_new = jnp.exp(score_new - top)
        total = jnp.sum(prob, axis=-1, keepdims=True) + jnp.sum(prob_new, axis=-1, keepdims=True)
        mixed = jnp.dot(prob.astype(bf16), vals, preferred_element_type=f32)
        mixed = (mixed + jnp.dot(prob_new.astype(bf16), val, preferred_element_type=f32)) / total
        stores = []
        for j in range(touched):
            page = pl.ds(pl.multiple_of(table_ref[b, first + j] * page_rows, page_rows), page_rows)
            piece = slice(j * page_rows, (j + 1) * page_rows)
            for c, cache in enumerate((kc, vc)):
                fill = new[piece, c * head_dim:(c + 1) * head_dim]
                old = cache[page, :].astype(f32)
                stores.append((c, j, page, jnp.where(fresh[piece], fill, old).astype(bf16)))
        return mine, mixed, stores


    def request_step(i, _):
        done = [attend(i * together + k) for k in range(together)]
        for k, (mine, mixed, stores) in enumerate(done):
            for h in range(heads):
                o_buf[mine, h * head_dim:(h + 1) * head_dim] = mixed[h * nodes:(h + 1) * nodes]
            for c, j, page, value in stores:
                slot = pl.ds(pl.multiple_of((i * together + k) * window + j * page_rows, page_rows), page_rows)
                renewed[c, slot, :] = value

        @pl.when(i == 0)
        def _():
            for whole in flush:
                whole.wait()

        for k, (mine, mixed, stores) in enumerate(done):
            for c, j, page, value in stores:
                slot = pl.ds(pl.multiple_of((i * together + k) * window + j * page_rows, page_rows), page_rows)
                out = (k_out, v_out)[c]
                pltpu.make_async_copy(renewed.at[c, slot, :], out.at[page, :], out_sems.at[2 + c]).start()
        return 0

    lax.fori_loop(0, requests // together, request_step, 0)
    att_ref[...] = o_buf[...].astype(bf16)
    att_copy = pltpu.make_async_copy(att_ref, att_out, small_sems.at[4])
    att_copy.start()
    for c, out in enumerate((k_out, v_out)):
        pltpu.make_async_copy(renewed.at[c], out.at[pl.ds(0, requests * window), :], out_sems.at[2 + c]).wait()
    att_copy.wait()


def attention(hidden, tree_mask, depth, ctx_len, block_table, freq, k_pages, v_pages, attn_norm, w_q, w_k, w_v, dims):
    requests, nodes, pages, page_rows, heads, head_dim = dims
    rows = requests * nodes
    model = hidden.shape[1]
    width = heads * head_dim
    bf16, f32 = jnp.bfloat16, jnp.float32
    window = window_pages(nodes, page_rows // heads) * page_rows
    scratch = [
        pltpu.VMEM(depth.shape, jnp.int32),
        pltpu.VMEM(freq.shape, f32),
        pltpu.VMEM(attn_norm.shape, bf16),
        pltpu.VMEM(tree_mask.shape, jnp.int32),
        pltpu.VMEM((rows, width), bf16),
        pltpu.VMEM((rows, model), bf16),
        pltpu.VMEM((rows, model), bf16),
        pltpu.VMEM((3, model, width), bf16),
        pltpu.VMEM(k_pages.shape, bf16),
        pltpu.VMEM(v_pages.shape, bf16),
        pltpu.VMEM((rows, head_dim), f32),
        pltpu.VMEM((rows, head_dim), f32),
        pltpu.VMEM((1, model), f32),
        pltpu.VMEM((heads * nodes, pages * page_rows), f32),
    ] + [pltpu.VMEM((rows, width), f32)] * 4 + [pltpu.VMEM((2, requests * window, head_dim), bf16), pltpu.SemaphoreType.DMA((7,)), pltpu.SemaphoreType.DMA((4,)), pltpu.SemaphoreType.DMA((5,))]
    return pl.pallas_call(
        functools.partial(attention_kernel, dims),
        name="attend",
        out_shape=(
            jax.ShapeDtypeStruct((rows, width), bf16),
            jax.ShapeDtypeStruct(k_pages.shape, bf16),
            jax.ShapeDtypeStruct(v_pages.shape, bf16),
        ),
        in_specs=[SMEM, SMEM] + [HBM] * 10,
        out_specs=(HBM, HBM, HBM),
        scratch_shapes=scratch,
        compiler_params=pltpu.CompilerParams(vmem_limit_bytes=VMEM_LIMIT),
    )(ctx_len, block_table, depth, freq, hidden, attn_norm, tree_mask, w_q, w_k, w_v, k_pages, v_pages)


def tail_kernel(
    chips, att_hbm, hid_hbm, mlp_gain_hbm, fin_gain_hbm, score_hbm, wo_hbm, wg_hbm, wu_hbm, wd_hbm, lm_hbm,
    top_ref, total_ref, pick_ref, att_ref, mlp_gain_ref, fin_gain_ref, score_ref, part, sib_in, rel_l, rel_r, in_l, in_r, xg, act, hid_own, run_max, run_sum, run_pick, stats, want_ref, gains,
    send_sems, recv_sems, stat_send, stat_recv, w_sems, wo_sems, lm_sems, hid_sem, small_sems,
):
    f32, bf16 = jnp.float32, jnp.bfloat16
    rows, model = xg.shape
    ffn = wg_hbm.shape[0]
    vocab = lm_hbm.shape[0]
    members = 2 * chips
    size = rows // members
    quarter = size * chips
    wide = model // STEPS
    sub = wide // 2
    me = lax.axis_index("tp")
    x = me // 2
    core = me % 2
    right = lax.rem(x + 1, chips) * 2 + core
    left = lax.rem(x + chips - 1, chips) * 2 + core
    sib = x * 2 + 1 - core

    barrier = pltpu.get_barrier_semaphore()
    for k in range(1, members):
        pl.semaphore_signal(barrier, inc=1, device_id={"tp": lax.rem(me + k, members)}, device_id_type=pl.DeviceIdType.MESH)

    def first_row(hop):
        return (core * chips + lax.rem(x + hop + chips, chips)) * size

    def block(hop):
        return pl.ds(pl.multiple_of(first_row(hop), 16), size)

    def lanes_of(start, width):
        return pl.ds(start if isinstance(start, int) else pl.multiple_of(start, 128), width)

    def cols(c, part=None):
        if part is None:
            return lanes_of(c * wide, wide)
        return lanes_of(c * wide + part * sub, sub)

    def plan(phase, c, name):
        far = pl.ds(pl.multiple_of((1 - core) * quarter, 16), quarter)
        own, opp, rgt, lft = block(0), block(2), block(1), block(-1)
        both = cols(c)
        c0, c1, here = cols(c, 0), cols(c, 1), lanes_of(c * sub, sub)
        entries = [
            ("pair", part.at[far, both], sib_in.at[:, both], sib),
            ("relay_r", part.at[opp, c0], rel_l.at[:, here], right),
            ("relay_l", part.at[opp, c1], rel_r.at[:, here], left),
            ("direct_r", part.at[rgt, c1], in_l.at[:, c1], right),
            ("direct_l", part.at[lft, c0], in_r.at[:, c0], left),
            ("acc_r", part.at[rgt, c0], in_l.at[:, c0], right),
            ("acc_l", part.at[lft, c1], in_r.at[:, c1], left),
            ("own_r0", xg.at[own, c0], xg.at[own, c0], right),
            ("own_l1", xg.at[own, c1], xg.at[own, c1], left),
            ("own_r1", xg.at[own, c1], xg.at[own, c1], right),
            ("own_l0", xg.at[own, c0], xg.at[own, c0], left),
            ("own_s", xg.at[own, both], xg.at[own, both], sib),
            ("fwd_r", xg.at[lft, c0], xg.at[lft, c0], right),
            ("fwd_l", xg.at[rgt, c1], xg.at[rgt, c1], left),
            ("lft_s", xg.at[lft, both], xg.at[lft, both], sib),
            ("rgt_s", xg.at[rgt, both], xg.at[rgt, both], sib),
            ("opp_s", xg.at[opp, both], xg.at[opp, both], sib),
        ]
        i = [entry[0] for entry in entries].index(name)
        _, src, dst, to = entries[i]
        return pltpu.make_async_remote_copy(
            src_ref=src, dst_ref=dst, send_sem=send_sems.at[phase, c, i], recv_sem=recv_sems.at[phase, c, i],
            device_id={"tp": to}, device_id_type=pl.DeviceIdType.MESH,
        )

    reduce_names = ("pair", "relay_r", "relay_l", "direct_r", "direct_l", "acc_r", "acc_l")
    own_names = ("own_r0", "own_l1", "own_r1", "own_l0", "own_s")
    other_names = ("fwd_r", "fwd_l", "lft_s", "rgt_s", "opp_s")
    steps = range(STEPS)

    def pair_sum(phase, c):
        both = cols(c)
        plan(phase, c, "pair").wait_recv()

        def add(i, _):
            there = pl.ds(pl.multiple_of(core * quarter + i * 32, 16), 32)
            here = pl.ds(pl.multiple_of(i * 32, 32), 32)
            part[there, both] = (part[there, both].astype(f32) + sib_in[here, both].astype(f32)).astype(bf16)
            return 0

        lax.fori_loop(0, quarter // 32, add, 0)
        for name in ("relay_r", "relay_l", "direct_r", "direct_l"):
            plan(phase, c, name).start()

    def accumulate(phase, c):
        here = lanes_of(c * sub, sub)
        for name, hop, which, buf in (("r", 1, 0, rel_l), ("l", -1, 1, rel_r)):
            plan(phase, c, f"relay_{name}").wait_recv()
            at = block(hop)
            part[at, cols(c, which)] = (part[at, cols(c, which)].astype(f32) + buf[:, here].astype(f32)).astype(bf16)
            plan(phase, c, f"acc_{name}").start()

    def own_send(phase, c):
        for name in own_names:
            plan(phase, c, name).start()

    def finish(phase):
        squares = 0.0
        for c in steps:
            both = cols(c)
            for name in ("direct_r", "direct_l", "acc_r", "acc_l"):
                plan(phase, c, name).wait_recv()
            total = part[block(0), both].astype(f32) + in_l[:, both].astype(f32) + in_r[:, both].astype(f32)
            residual = (hid_own[:, both].astype(f32) + total.astype(bf16).astype(f32)).astype(bf16)
            hid_own[:, both] = residual
            full = residual.astype(f32)
            squares = squares + jnp.sum(full * full, axis=-1, keepdims=True)
        scale = lax.rsqrt(squares * (1.0 / model) + RMS_EPS)
        for c in steps:
            both = cols(c)
            xg[block(0), both] = (hid_own[:, both].astype(f32) * scale * gains[phase:phase + 1, both]).astype(bf16)
            if c < 2:
                own_send(phase, c)

    def forward(phase, c, more=True):
        plan(phase, c, "own_r0").wait_recv()
        plan(phase, c, "fwd_r").start()
        plan(phase, c, "own_l1").wait_recv()
        plan(phase, c, "fwd_l").start()
        if more:
            own_send(phase, c + 2)

    def share(phase, c):
        plan(phase, c, "own_r1").wait_recv()
        plan(phase, c, "lft_s").start()
        plan(phase, c, "own_l0").wait_recv()
        plan(phase, c, "rgt_s").start()
        plan(phase, c, "fwd_r").wait_recv()
        plan(phase, c, "fwd_l").wait_recv()
        plan(phase, c, "opp_s").start()

    def ready(phase, c):
        for name in ("own_s", "lft_s", "rgt_s", "opp_s"):
            plan(phase, c, name).wait_recv()

    def drain(phase):
        def one(c, _):
            for name in reduce_names + own_names + other_names:
                plan(phase, c, name).wait_send()
            return 0

        lax.fori_loop(0, STEPS, one, 0)

    def reduce_start(phase, lhs_ref, w_ref, before):
        def step(c, _):
            before(c)
            part[:, cols(c)] = jnp.dot(lhs_ref[...], w_ref[:, cols(c)], preferred_element_type=f32).astype(bf16)
            plan(phase, c, "pair").start()

            @pl.when(c >= 1)
            def _():
                pair_sum(phase, c - 1)

            @pl.when(c >= 3)
            def _():
                accumulate(phase, c - 3)

            return 0

        lax.fori_loop(0, STEPS, step, 0)

    def reduce_end(phase, filler):
        def step(c, _):
            @pl.when(c <= STEPS)
            def _():
                pair_sum(phase, c - 1)

            accumulate(phase, c - 3)
            return 0

        lax.fori_loop(STEPS, STEPS + 3, step, 0)
        filler()
        finish(phase)

    def gather(phase, compute, loads, early):
        forward(phase, 0)
        forward(phase, 1)
        share(phase, 0)
        ready(phase, 0)
        forward(phase, 2, False)
        for load in loads:
            load.wait()

        def step(c, _):
            compute(cols(c), False, 0)

            @pl.when(c <= 1)
            def _():
                share(phase, c + 1)

            @pl.when(c == 0)
            def _():
                forward(phase, 3, False)

            compute(cols(c), False, 1)

            @pl.when(c == 1)
            def _():
                share(phase, 3)

            @pl.when(c + 1 < early)
            def _():
                ready(phase, c + 1)

            return 0

        lax.fori_loop(0, early, step, 0)
        for c in range(early, STEPS):
            ready(phase, c)
        compute(pl.ds(early * wide, (STEPS - early) * wide), True, None)

    def layer(wo, wg, wu, wd, gate_acc, up_acc):
        loads = [
            pltpu.make_async_copy(src, dst, w_sems.at[i])
            for i, (src, dst) in enumerate(((wg_hbm, wg), (wu_hbm, wu), (wd_hbm, wd)))
        ]
        def wo_piece(c):
            return pltpu.make_async_copy(wo_hbm.at[:, cols(c)], wo.at[:, cols(c)], wo_sems.at[c])

        small = [
            pltpu.make_async_copy(src, dst, small_sems.at[i])
            for i, (src, dst) in enumerate((
                (att_hbm, att_ref), (mlp_gain_hbm, mlp_gain_ref), (fin_gain_hbm, fin_gain_ref), (score_hbm, score_ref),
            ))
        ]
        small[0].start()
        for c in steps:
            wo_piece(c).start()
        for copy in small[1:]:
            copy.start()
        own_rows = pltpu.make_async_copy(hid_hbm.at[block(0), :], hid_own, hid_sem.at[0])
        own_rows.start()

        def before(c):
            wo_piece(c).wait()

            @pl.when(c == STEPS - 1)
            def _():
                for load in loads:
                    load.start()

        def filler():
            for copy in small[1:]:
                copy.wait()
            gains[0:1, :] = gain_row(mlp_gain_ref)
            gains[1:2, :] = gain_row(fin_gain_ref)
            gate_acc[...] = jnp.zeros(gate_acc.shape, f32)
            up_acc[...] = jnp.zeros(up_acc.shape, f32)
            own_rows.wait()

        small[0].wait()
        pl.semaphore_wait(barrier, members - 1)
        reduce_start(0, att_ref, wo, before)
        reduce_end(0, filler)

        def gated(span, is_last, half):
            def close(start, width):
                at = pl.ds(start, width)
                gate = gate_acc[:, at]
                act[:, at] = (gate * jax.nn.sigmoid(gate) * up_acc[:, at]).astype(bf16)

            def tile(start, width):
                at = pl.ds(start, width)
                for w, acc in ((wg, gate_acc), (wu, up_acc)):
                    acc[:, at] += lax.dot_general(xg[:, span], w[at, span], LAST, preferred_element_type=f32)

            def step(t, _):
                tile(pl.multiple_of(t * GATE, GATE), GATE)
                return 0

            full = ffn // GATE
            if is_last:
                pieces = [(t * GATE, min(GATE, ffn - t * GATE)) for t in range(-(-ffn // GATE))]
                tile(*pieces[0])
                for t in range(1, len(pieces)):
                    close(*pieces[t - 1])
                    tile(*pieces[t])
                close(*pieces[-1])
            elif half == 0:
                lax.fori_loop(0, full, step, 0)
            else:
                tile(full * GATE, ffn - full * GATE)

        gather(0, gated, loads[:2], STEPS - 1)
        drain(0)
        loads[2].wait()
        reduce_start(1, act, wd, lambda c: None)

    pl.run_scoped(
        layer,
        pltpu.VMEM(wo_hbm.shape, bf16), pltpu.VMEM((ffn, model), bf16), pltpu.VMEM((ffn, model), bf16), pltpu.VMEM((ffn, model), bf16),
        pltpu.VMEM((rows, ffn), f32), pltpu.VMEM((rows, ffn), f32),
    )

    pieces = 5
    lanes = 128

    def head(lm, acc):
        loads = []
        step_rows = vocab // pieces
        for i in range(pieces):
            piece = pl.ds(i * step_rows, step_rows)
            loads.append(pltpu.make_async_copy(lm_hbm.at[piece, :], lm.at[piece, :], lm_sems.at[i]))
            loads[-1].start()

        def want_step(b, _):
            nodes = score_ref.shape[1]
            column = column_of(score_ref, b).astype(jnp.int32)
            want_ref[pl.ds(pl.multiple_of(b * nodes, 8), nodes), :] = jnp.broadcast_to(column, (nodes, 128))
            return 0

        run_max[...] = jnp.full(run_max.shape, -jnp.inf, f32)
        run_sum[...] = jnp.zeros(run_sum.shape, f32)
        run_pick[...] = jnp.zeros(run_pick.shape, f32)
        full = vocab // HEAD
        rest = vocab % HEAD
        whole = rest // lanes * lanes

        def fold(base, width):
            parts = [acc[:, pl.ds(base + i * lanes, lanes)] for i in range(width // lanes)]
            old = run_max[...]
            new = functools.reduce(jnp.maximum, parts, old)
            lane = lax.broadcasted_iota(jnp.int32, (1, lanes), 1) + base + me * vocab
            want = want_ref[...]
            total = run_sum[...] * jnp.exp(old - new)
            pick = run_pick[...]
            for i, one in enumerate(parts):
                total = total + jnp.exp(one - new)
                pick = pick + jnp.where(lane + i * lanes == want, one, 0.0)
            run_max[...] = new
            run_sum[...] = total
            run_pick[...] = pick

        def logits(span, is_last, half):
            def tile(base, width):
                at = pl.ds(base, width)
                acc[:, at] += lax.dot_general(xg[:, span], lm[at, span], LAST, preferred_element_type=f32)

            def step(t, _):
                tile(pl.multiple_of(t * HEAD, HEAD), HEAD)
                return 0

            cut = (full + 1) // 2
            if is_last:
                for t in range(full):
                    tile(t * HEAD, HEAD)
                    if t > 0:
                        fold((t - 1) * HEAD, HEAD)
                fold((full - 1) * HEAD, HEAD)
                tile(full * HEAD, rest)
            elif half == 0:
                lax.fori_loop(0, cut, step, 0)
            else:
                lax.fori_loop(cut, full, step, 0)
                tile(full * HEAD, rest)

        def filler():
            lax.fori_loop(0, score_ref.shape[0], want_step, 0)
            acc[...] = jnp.zeros(acc.shape, f32)

        reduce_end(1, filler)
        gather(1, logits, loads, STEPS - 2)
        fold(full * HEAD, whole)
        end = acc[:, full * HEAD + whole:vocab]
        top = jnp.maximum(jnp.max(run_max[...], axis=-1, keepdims=True), jnp.max(end, axis=-1, keepdims=True))
        total = jnp.sum(run_sum[...] * jnp.exp(run_max[...] - top), axis=-1, keepdims=True)
        total = total + jnp.sum(jnp.exp(end - top), axis=-1, keepdims=True)
        lane = lax.broadcasted_iota(jnp.int32, (1, rest - whole), 1) + (full * HEAD + whole) + me * vocab
        pick = jnp.sum(run_pick[...], axis=-1, keepdims=True)
        pick = pick + jnp.sum(jnp.where(lane == want_ref[:, 0:1], end, 0.0), axis=-1, keepdims=True)
        place = lax.broadcasted_iota(jnp.int32, (1, lanes), 1)
        packed = jnp.where(place == 0, top, jnp.where(place == 1, total, pick))
        stats[me] = packed.T[0:8, :]

    pl.run_scoped(head, pltpu.VMEM((vocab, model), bf16), pltpu.VMEM((rows, vocab), f32))

    sends = []
    for k in range(1, members):
        to = lax.rem(me + k, members)
        sends.append(pltpu.make_async_remote_copy(
            src_ref=stats.at[me], dst_ref=stats.at[me], send_sem=stat_send.at[k - 1], recv_sem=stat_recv.at[k - 1],
            device_id={"tp": to}, device_id_type=pl.DeviceIdType.MESH,
        ))
        sends[-1].start()
    drain(1)
    for copy in sends:
        copy.wait()
    every = [stats[i] for i in range(members)]
    top = functools.reduce(jnp.maximum, [e[0:1, :] for e in every])
    total = functools.reduce(jnp.add, [e[1:2, :] * jnp.exp(e[0:1, :] - top) for e in every])
    pick = functools.reduce(jnp.add, [e[2:3, :] for e in every])
    requests, nodes = score_ref.shape
    for b in range(requests):
        for ref, row in ((top_ref, top), (total_ref, total), (pick_ref, pick)):
            ref[b:b + 1, :] = row[:, b * nodes:(b + 1) * nodes]


def tail(attended, hidden, mlp_norm, final_norm, score_id, w_o, w_gate, w_up, w_down, w_lm, chips):
    rows, model = hidden.shape
    ffn = w_gate.shape[0]
    members = 2 * chips
    bf16, f32 = jnp.bfloat16, jnp.float32
    own = rows // members
    scratch = [
        pltpu.VMEM(attended.shape, bf16),
        pltpu.VMEM(mlp_norm.shape, bf16),
        pltpu.VMEM(final_norm.shape, bf16),
        pltpu.VMEM(score_id.shape, jnp.int32),
        pltpu.VMEM((rows, model), bf16),
        pltpu.VMEM((rows // 2, model), bf16),
        pltpu.VMEM((own, model // 2), bf16),
        pltpu.VMEM((own, model // 2), bf16),
        pltpu.VMEM((own, model), bf16),
        pltpu.VMEM((own, model), bf16),
        pltpu.VMEM((rows, model), bf16),
        pltpu.VMEM((rows, ffn), bf16),
        pltpu.VMEM((own, model), bf16),
        pltpu.VMEM((rows, 128), f32),
        pltpu.VMEM((rows, 128), f32),
        pltpu.VMEM((rows, 128), f32),
        pltpu.VMEM((members, 8, rows), f32),
        pltpu.VMEM((rows, 128), jnp.int32),
        pltpu.VMEM((2, model), f32),
        pltpu.SemaphoreType.DMA((2, STEPS, 17)),
        pltpu.SemaphoreType.DMA((2, STEPS, 17)),
        pltpu.SemaphoreType.DMA((members - 1,)),
        pltpu.SemaphoreType.DMA((members - 1,)),
        pltpu.SemaphoreType.DMA((3,)),
        pltpu.SemaphoreType.DMA((STEPS,)),
        pltpu.SemaphoreType.DMA((5,)),
        pltpu.SemaphoreType.DMA((1,)),
        pltpu.SemaphoreType.DMA((4,)),
    ]
    return pl.pallas_call(
        functools.partial(tail_kernel, chips),
        name="tail",
        out_shape=(jax.ShapeDtypeStruct(score_id.shape, f32),) * 3,
        in_specs=[HBM] * 10,
        out_specs=(VMEM, VMEM, VMEM),
        scratch_shapes=scratch,
        compiler_params=pltpu.CompilerParams(vmem_limit_bytes=VMEM_LIMIT, collective_id=0, has_side_effects=True),
    )(attended, hidden, mlp_norm, final_norm, score_id, w_o, w_gate, w_up, w_down, w_lm)


def solution(mesh):
    chips = mesh.shape["tp"] // 2

    def group_step(hidden, tree_mask, depth, ctx_len, block_table, score_id, k_cache, v_cache, attn_norm, w_q, w_k, w_v, w_o, mlp_norm, w_gate, w_up, w_down, final_norm, w_lm):
        requests, nodes, model = hidden.shape
        blocks, page_size, heads, head_dim = k_cache.shape
        dims = (requests, nodes, block_table.shape[1], page_size * heads, heads, head_dim)
        rows = requests * nodes
        flat = hidden.reshape(rows, model)
        inv_freq = 1.0 / (ROPE_THETA ** (np.arange(head_dim // 2) * (2.0 / head_dim)))
        freq = jnp.asarray(np.concatenate([inv_freq, inv_freq])[None, :], jnp.float32)
        pages = (blocks * page_size * heads, head_dim)
        attended, k_out, v_out = attention(
            flat, tree_mask, depth, ctx_len, block_table, freq, k_cache.reshape(pages), v_cache.reshape(pages),
            attn_norm.reshape(model // 128, 128), w_q, w_k, w_v, dims,
        )
        top, total, pick = tail(
            attended, flat, mlp_norm.reshape(model // 128, 128), final_norm.reshape(model // 128, 128), score_id,
            w_o, w_gate.T, w_up.T, w_down, w_lm.T, chips,
        )
        log_norm = top + jnp.log(total)
        return log_norm, pick - log_norm, k_out.reshape(k_cache.shape), v_out.reshape(v_cache.shape)

    request_spec = P("dp", None, None)
    node_spec = P("dp", None)
    cache_spec = P("dp", None, "tp", None)
    shared_spec = P(None)
    column_spec = P(None, "tp")
    row_spec = P("tp", None)
    in_specs = (request_spec, request_spec, node_spec, P("dp"), node_spec, node_spec, cache_spec, cache_spec, shared_spec, column_spec, column_spec, column_spec, row_spec, shared_spec, column_spec, column_spec, row_spec, shared_spec, column_spec)
    out_specs = (node_spec, node_spec, cache_spec, cache_spec)
    return jax.shard_map(group_step, mesh=mesh, in_specs=in_specs, out_specs=out_specs, check_vma=False)
```
